768 devices in a mesh: mem: 48 (over z, y_lo, core), slab: 16 (over x, y_hi).
Axes of the slice: x: 4, y: 8 (y_hi: 4, y_lo: 2; y = y_hi * 2 + y_lo), z: 12, core: 2. Of those that a mesh axis runs over, the one named last changes fastest.
Arguments:
- thickness: float32 [384, 1024, 384], P('mem', 'slab'), may hold values from 0.5 to 2.5
- face_u: float32 [1024, 384], P('slab'), may hold values from -0.4 to 0.4
- face_v: float32 [1024, 384], P('slab'), may hold values from -0.4 to 0.4
- obs_cells: int32 [2048, 4], P('slab'), may hold values from 0 to 393215, as said below
- obs_weights: int32 [2048, 4], P('slab'), may hold values from 1 to 4
- obs_values: float32 [2048], P('slab'), may hold values from -6 to 6
- obs_noise: float32 [384, 2048], P('mem', 'slab'), may hold values from -3 to 3
- cov_inverse: float32 [2048, 2048], P('slab'), may hold values from -0.1875 to 0.1875
- taper_mask: int32 [16, 16], replicated, may hold values from 0 to 1, as said below
Outputs:
- analysis: float32 [384, 1024, 384], P('mem', 'slab')
The draws below stay inside these ranges and needn't reach their ends.
Inputs may be any that keep to these rules, and one draw needn't show every extreme that they name: `obs_cells`: observation o covers a 2 x 2 square of cells, all within the rows of slab o // 128. `taper_mask`: entries are 0 or 1 and the diagonal is 1.
All inputs are finite; a program needn't handle non-finite values.
Results may differ from the reference program's by a relative error of at most 0.0003.
Values sent between devices are 32-bit elements; how exact they have to be, the bound alone decides.
No kernel may reach another device: no remote copies, remote signals or barrier semaphores. Data moves between devices by JAX's collectives and lax.ppermute only.
A program may use at most 64 MiB of HBM per device.

```python
import jax
import jax.numpy as jnp
from jax import lax

ROWS_SLAB = 64
CELLS_PER_ROW = 384
OBS_SLAB = 128
FOOT = 4
ENSEMBLE_SIZE = 384
GRID_ROWS = 1024
OBS = 2048
N_SLAB = 16


def draw_obs_cells(key, part):
    key_row, key_col = jax.random.split(jax.random.fold_in(key, 11))
    block_of = jnp.arange(OBS, dtype=jnp.int32) // OBS_SLAB
    row_base = block_of * ROWS_SLAB + jax.random.randint(key_row, (OBS,), 0, ROWS_SLAB - 1)
    col_base = jax.random.randint(key_col, (OBS,), 0, CELLS_PER_ROW - 1)
    row_offset = jnp.array([0, 0, 1, 1], dtype=jnp.int32)
    col_offset = jnp.array([0, 1, 0, 1], dtype=jnp.int32)
    cells_flat = (row_base[:, None] + row_offset[None, :]) * CELLS_PER_ROW + col_base[:, None] + col_offset[None, :]
    return cells_flat.astype(jnp.int32)


def draw_taper_mask(key, part):
    coin_flips = jax.random.randint(jax.random.fold_in(key, 23), (N_SLAB, N_SLAB), 0, 2)
    diagonal = jnp.eye(N_SLAB, dtype=jnp.int32)
    return jnp.maximum(coin_flips, diagonal).astype(jnp.int32)


def with_ends(values, rng, smallest, high):
    index_at = [jax.random.randint(jax.random.fold_in(rng, axis), (), 0, length) for axis, length in enumerate(values.shape)]
    widest = values.shape.index(max(values.shape))
    next_to = index_at[:widest] + [(index_at[widest] + 1) % values.shape[widest]] + index_at[widest + 1:]
    return values.at[tuple(index_at)].set(smallest).at[tuple(next_to)].set(high)


def with_spikes(result, stream_key, source, target, shards_of, factor):
    owner, partner = [(jnp.arange(result.shape[axis_at]) // (result.shape[axis_at] // shards_of)).reshape([-1 if axis == axis_at else 1 for axis in range(result.ndim)]) for axis_at in (source, target)]
    chosen = jax.random.permutation(stream_key, shards_of)[partner]
    strong = (owner == chosen) | (owner == (partner + shards_of // 2) % shards_of)
    return jnp.where(strong, factor * result, result)


def shard_levels(stream_key, dims, shards, low, high):
    level, own = 1.0, jax.random.fold_in(stream_key, 6)
    for dim, blocks in shards:
        steps = jnp.exp(jax.random.uniform(jax.random.fold_in(own, dim), (blocks,), jnp.float32, low / len(shards), high / len(shards)))
        level = level * jnp.repeat(steps, dims[dim] // blocks).reshape([-1 if axis == dim else 1 for axis in range(len(dims))])
    return level


def scatter_about(key, extent, width, most, cuts=(), kind=jnp.bfloat16):
    entries = width * jax.random.normal(key, extent, jnp.float32)
    if cuts:
        entries = entries * shard_levels(key, extent, cuts, -0.22, 0.18)
    return jnp.clip(entries, -most, most).astype(kind)


def heavy_noise(rng, extent, scale, bound, pieces, heavy, kind=jnp.bfloat16):
    entries = scale * jax.random.normal(rng, extent, jnp.float32)
    if pieces:
        entries = entries * shard_levels(rng, extent, pieces, -0.22, 0.18)
    return jnp.clip(with_spikes(entries, jax.random.fold_in(rng, 3), *heavy), -bound, bound).astype(kind)


def setup_inputs(seed: int = 0) -> dict:
    streams_of = jax.random.split(jax.random.key(seed), 10)
    return {
        "thickness": jnp.clip(0.5 + 2.0 * jax.random.uniform(streams_of[0], (ENSEMBLE_SIZE, GRID_ROWS, CELLS_PER_ROW), jnp.float32) ** shard_levels(streams_of[0], (ENSEMBLE_SIZE, GRID_ROWS, CELLS_PER_ROW), ((0, 48), (1, 16)), -0.2, 0.2), 0.5, 2.5),
        "face_u": jnp.clip(jax.random.uniform(streams_of[1], (GRID_ROWS, CELLS_PER_ROW), jnp.float32, -0.4, 0.4) * shard_levels(streams_of[1], (GRID_ROWS, CELLS_PER_ROW), ((0, 16),), -0.4, 0.0), -0.4, 0.4),
        "face_v": jnp.clip(jax.random.uniform(streams_of[2], (GRID_ROWS, CELLS_PER_ROW), jnp.float32, -0.4, 0.4) * shard_levels(streams_of[2], (GRID_ROWS, CELLS_PER_ROW), ((0, 16),), -0.4, 0.0), -0.4, 0.4),
        "obs_cells": draw_obs_cells(jax.random.fold_in(streams_of[9], 71), 0),
        "obs_weights": with_ends(jax.random.randint(streams_of[4], (OBS, FOOT), 1, 5), jax.random.fold_in(streams_of[4], 1), 1, 4).astype(jnp.int32),
        "obs_values": scatter_about(streams_of[5], (OBS,), 1.0, 6.0, ((0, 16),), jnp.float32),
        "obs_noise": scatter_about(streams_of[6], (ENSEMBLE_SIZE, OBS), 0.5, 3.0, ((0, 48), (1, 16)), jnp.float32),
        "cov_inverse": heavy_noise(streams_of[7], (OBS, OBS), OBS ** -0.5, 0.1875, ((0, 16),), (0, 1, 16, 2.0), jnp.float32),
        "taper_mask": draw_taper_mask(jax.random.fold_in(streams_of[9], 71), 0),
    }


def minmod(first_diff, second_diff):
    return 0.5 * (jnp.sign(first_diff) + jnp.sign(second_diff)) * jnp.minimum(jnp.abs(first_diff), jnp.abs(second_diff))


def face_flux(padded, velocity, axis_dim):
    counted = padded.shape[axis_dim] - 3
    far_low = lax.slice_in_dim(padded, 0, counted, axis=axis_dim)
    near_low = lax.slice_in_dim(padded, 1, 1 + counted, axis=axis_dim)
    near_high = lax.slice_in_dim(padded, 2, 2 + counted, axis=axis_dim)
    far_high = lax.slice_in_dim(padded, 3, 3 + counted, axis=axis_dim)
    left_state = near_low + 0.5 * minmod(near_low - far_low, near_high - near_low)
    right_state = near_high - 0.5 * minmod(near_high - near_low, far_high - near_high)
    return jnp.maximum(velocity, 0.0) * left_state + jnp.minimum(velocity, 0.0) * right_state


def reference(thickness, face_u, face_v, obs_cells, obs_weights, obs_values, obs_noise, cov_inverse, taper_mask):
    ftype = thickness.dtype
    row_pad = jnp.pad(thickness, ((0, 0), (2, 2), (0, 0)))
    row_speed = jnp.concatenate([face_v, jnp.zeros((1, CELLS_PER_ROW), ftype)], 0)
    row_fluxes = face_flux(row_pad, row_speed, 1)
    col_pad = jnp.pad(thickness, ((0, 0), (0, 0), (2, 2)))
    col_speed = jnp.concatenate([face_u, jnp.zeros((GRID_ROWS, 1), ftype)], 1)
    column_fluxes = face_flux(col_pad, col_speed, 2)
    prior_state = thickness - (column_fluxes[:, :, 1:] - column_fluxes[:, :, :-1]) - (row_fluxes[:, 1:, :] - row_fluxes[:, :-1, :])
    state_vector = prior_state.reshape(ENSEMBLE_SIZE, GRID_ROWS * CELLS_PER_ROW)
    weights = obs_weights.astype(ftype)
    picked = state_vector[:, obs_cells]
    obs_model = jnp.sum(picked * weights[None], -1) / jnp.sum(weights, -1)[None]
    innovation = obs_values[None, :] + obs_noise - obs_model
    whitened = jnp.dot(innovation, cov_inverse, precision=lax.Precision.HIGHEST)
    obs_anomaly = obs_model - jnp.mean(obs_model, 0, keepdims=True)
    anomaly = state_vector - jnp.mean(state_vector, 0, keepdims=True)
    anom_blocks = obs_anomaly.reshape(ENSEMBLE_SIZE, N_SLAB, OBS_SLAB)
    white_blocks = whitened.reshape(ENSEMBLE_SIZE, N_SLAB, OBS_SLAB)
    block_products = jnp.einsum("mbo,nbo->bmn", anom_blocks, white_blocks, precision=lax.Precision.HIGHEST)
    ensemble = jnp.einsum("sb,bmn->smn", taper_mask.astype(ftype), block_products, precision=lax.Precision.HIGHEST)
    anom_slabs = anomaly.reshape(ENSEMBLE_SIZE, N_SLAB, ROWS_SLAB * CELLS_PER_ROW)
    update = jnp.einsum("smn,msc->nsc", ensemble, anom_slabs, precision=lax.Precision.HIGHEST) / (ENSEMBLE_SIZE - 1)
    analysis = state_vector + update.reshape(ENSEMBLE_SIZE, GRID_ROWS * CELLS_PER_ROW)
    return analysis.reshape(ENSEMBLE_SIZE, GRID_ROWS, CELLS_PER_ROW)
```

```python
import jax
import jax.numpy as jnp
from jax import lax
from jax.experimental import pallas as pl
from jax.experimental.pallas import tpu as pltpu
from jax.sharding import PartitionSpec as P


LANES = 128
PLANE = 4
RUN = 4
COLUMN = 4
HIGHEST = lax.Precision.HIGHEST
SMEM = pltpu.SMEM
VMEM = pltpu.VMEM


def minmod(a, b):
    return jnp.maximum(jnp.minimum(a, b), 0.0) + jnp.minimum(jnp.maximum(a, b), 0.0)


def vspec():
    return pl.BlockSpec(memory_space=VMEM)


def sspec():
    return pl.BlockSpec(memory_space=SMEM)


def edges_kernel(first_ref, last_ref, v_ref, up_ref, down_ref):
    for r in range(2):
        up_ref[r] = first_ref[:, r, :]
        down_ref[r] = last_ref[:, 6 + r, :]
    up_ref[2] = jnp.broadcast_to(v_ref[0:1, :], up_ref.shape[1:])


def forecast_kernel(
    slab_ref, cells_ref, weights_ref, h_ref, low_ref, high_ref, u_ref, v_ref, values_ref, noise_ref, cov_ref,
    f_ref, obs_ref, white_ref,
):
    members = noise_ref.shape[0]
    rows, cols = u_ref.shape
    per_row = cols // LANES
    lane = lax.broadcasted_iota(jnp.int32, (members, cols), 1)
    at_first = lane == 0
    at_last = lane == cols - 1

    blocks = {}

    def row(r):
        if r // 8 not in blocks:
            blocks[r // 8] = jnp.swapaxes(h_ref[:, r // 8 * 8 : r // 8 * 8 + 8, :], 0, 1)
        return blocks[r // 8][r % 8]

    def columns_term(h, u):
        prev = jnp.where(at_first, 0.0, pltpu.roll(h, 1, 1))
        d = h - prev
        d_next = jnp.where(at_last, -h, pltpu.roll(d, cols - 1, 1))
        half = 0.5 * minmod(d, d_next)
        left = jnp.where(at_first, 0.0, pltpu.roll(h + half, 1, 1))
        flux = jnp.maximum(u, 0.0) * left + jnp.minimum(u, 0.0) * (h - half)
        flux_next = jnp.where(at_last, 0.0, pltpu.roll(flux, cols - 1, 1))
        return flux_next - flux

    def row_flux(v, h_low, half_low, h_high, half_high):
        return jnp.maximum(v, 0.0) * (h_low + half_low) + jnp.minimum(v, 0.0) * (h_high - half_high)

    low2, low1 = low_ref[0], low_ref[1]
    h0, h1 = row(0), row(1)
    d0, d1 = h0 - low1, h1 - h0
    half_low = 0.5 * minmod(low1 - low2, d0)
    half0 = 0.5 * minmod(d0, d1)
    flux0 = row_flux(v_ref[0:1, :], low1, half_low, h0, half0)
    carry = (h0, h1, d1, half0, flux0)
    for r in range(rows):
        h, h_up, d_up, half, flux = carry
        if r + 2 < rows:
            h_up2 = row(r + 2)
        else:
            h_up2 = high_ref[r + 2 - rows]
        v = v_ref[r + 1 : r + 2, :] if r + 1 < rows else high_ref[2, 0:1, :]
        d_up2 = h_up2 - h_up
        half_up = 0.5 * minmod(d_up, d_up2)
        flux_up = row_flux(v, h, half, h_up, half_up)
        f = h - columns_term(h, u_ref[r : r + 1, :]) - (flux_up - flux)
        for t in range(per_row):
            f_ref[r * per_row + t] = f[:, t * LANES : (t + 1) * LANES]
        carry = (h_up, h_up2, d_up2, half_up, flux_up)

    base = slab_ref[0] * (rows * cols)
    count = cells_ref.shape[0]
    foot = cells_ref.shape[1]
    lane1 = lax.broadcasted_iota(jnp.int32, (members, LANES), 1)

    def observe(o, carry):
        total, norm = carry
        acc = jnp.zeros((members, LANES), jnp.float32)
        wsum = jnp.float32(0.0)
        for k in range(foot):
            c = cells_ref[o, k] - base
            w = weights_ref[o, k].astype(jnp.float32)
            tile = f_ref[c >> 7]
            acc = acc + jnp.where(lane1 == (c & (LANES - 1)), w * tile, 0.0)
            wsum = wsum + w
        here = lane1 == o
        total = jnp.where(here, jnp.sum(acc, axis=1, keepdims=True), total)
        norm = jnp.where(here, wsum, norm)
        return total, norm

    init = jnp.zeros((members, LANES), jnp.float32)
    total, norm = lax.fori_loop(0, count, observe, (init, init + 1.0), unroll=8)
    obs = total / norm
    obs_ref[...] = obs
    innovation = values_ref[...] + noise_ref[...] - obs
    white = jnp.dot(innovation, cov_ref[...], precision=HIGHEST, preferred_element_type=jnp.float32)
    for s in range(white_ref.shape[0]):
        white_ref[s] = white[:, s * LANES : (s + 1) * LANES]


def products_kernel(obs_ref, white_ref, out_ref):
    a = obs_ref[...]
    a = a - jnp.mean(a, axis=0, keepdims=True)
    w = white_ref[0]
    for s in range(1, white_ref.shape[0]):
        w = w + white_ref[s]
    out_ref[...] = lax.dot_general(
        w, a, (((1,), (1,)), ((), ())), precision=HIGHEST, preferred_element_type=jnp.float32
    )


def tapered_kernel(slab_ref, mask_ref, x_ref, out_ref):
    slabs = mask_ref.shape[0]
    members = out_ref.shape[0]
    e = jnp.zeros(out_ref.shape, jnp.float32)
    for b in range(slabs):
        e = e + mask_ref[slab_ref[0], b].astype(jnp.float32) * x_ref[b * members : (b + 1) * members, :]
    out_ref[...] = e


def mixing_kernel(x_ref, e_ref, out_ref):
    mems, tiles, members, width = x_ref.shape
    total = mems * members
    e = e_ref[...]
    depth = mems // PLANE
    for t in range(tiles):
        x = x_ref[:, t].reshape(total, width)
        x = x - jnp.mean(x, axis=0, keepdims=True)
        u = jnp.dot(e, x, precision=HIGHEST, preferred_element_type=jnp.float32) / (total - 1)
        for q in range(PLANE):
            for z in range(depth):
                at = (q * depth + z) * members
                out_ref[z * PLANE + q, t] = u[at : at + members]


def add_kernel(f_ref, y_ref, out_ref):
    rows, cols = out_ref.shape[1:]
    per_row = cols // LANES
    for r in range(0, rows, 8):
        for t in range(per_row):
            at = [(r + i) * per_row + t for i in range(8)]
            tile = jnp.stack([f_ref[i] + y_ref[i] for i in at], 0)
            out_ref[:, r : r + 8, t * LANES : (t + 1) * LANES] = jnp.swapaxes(tile, 0, 1)


def f32(*shape):
    return jax.ShapeDtypeStruct(shape, jnp.float32)


def gathered(x, axis, groups):
    return lax.all_gather(x, axis, axis=0, tiled=True, axis_index_groups=groups)


def local(
    thickness, face_u, face_v, obs_cells, obs_weights, obs_values, obs_noise, cov_inverse, taper_mask,
):
    members, rows, cols = thickness.shape
    mems = lax.axis_size("mem")
    slabs = lax.axis_size("slab")
    depth = mems // PLANE
    tiles = rows * cols // LANES
    slab = lax.axis_index("slab").astype(jnp.int32).reshape(1)
    planes = [[z * PLANE + q for q in range(PLANE)] for z in range(depth)]
    runs = [
        [(z0 + z) * PLANE + q for z in range(RUN)] for z0 in range(0, depth, RUN) for q in range(PLANE)
    ]
    strides = [
        [(z0 + z) * PLANE + q for z0 in range(0, depth, RUN)] for z in range(RUN) for q in range(PLANE)
    ]
    along_y = [[x * COLUMN + y for y in range(COLUMN)] for x in range(slabs // COLUMN)]
    along_x = [[x * COLUMN + y for x in range(slabs // COLUMN)] for y in range(COLUMN)]

    up, down = pl.pallas_call(
        edges_kernel,
        grid=(1,),
        in_specs=[
            pl.BlockSpec((members, 8, cols), lambda i: (0, 0, 0)),
            pl.BlockSpec((members, 8, cols), lambda i: (0, rows // 8 - 1, 0)),
            pl.BlockSpec((8, cols), lambda i: (0, 0)),
        ],
        out_specs=[
            pl.BlockSpec((3, members, cols), lambda i: (0, 0, 0)),
            pl.BlockSpec((2, members, cols), lambda i: (0, 0, 0)),
        ],
        out_shape=[f32(3, members, cols), f32(2, members, cols)],
        name="edges",
    )(thickness, thickness, face_v)
    low = lax.ppermute(down, "slab", [(i, i + 1) for i in range(slabs - 1)])
    high = lax.ppermute(up, "slab", [(i + 1, i) for i in range(slabs - 1)])

    forecast, obs_model, white_terms = pl.pallas_call(
        forecast_kernel,
        in_specs=[sspec(), sspec(), sspec()] + [vspec() for _ in range(8)],
        out_specs=[vspec() for _ in range(3)],
        out_shape=[f32(tiles, members, LANES), f32(members, LANES), f32(slabs, members, LANES)],
        name="forecast",
    )(
        slab, obs_cells, obs_weights, thickness, low, high, face_u, face_v,
        obs_values.reshape(1, -1), obs_noise, cov_inverse,
    )

    white_arrived = lax.all_to_all(white_terms, "slab", 0, 0, tiled=True)
    obs_all = gathered(gathered(gathered(obs_model, "mem", planes), "mem", runs), "mem", strides)
    cell_state = lax.all_to_all(
        forecast.reshape(mems, tiles // mems, members, LANES), "mem", 0, 0, tiled=True
    )
    product = pl.pallas_call(
        products_kernel,
        in_specs=[vspec(), vspec()],
        out_specs=vspec(),
        out_shape=f32(members, mems * members),
        name="products",
    )(obs_all, white_arrived)
    blocks = gathered(gathered(product, "slab", along_y), "slab", along_x)
    own_rows = pl.pallas_call(
        tapered_kernel,
        in_specs=[sspec(), sspec(), vspec()],
        out_specs=vspec(),
        out_shape=f32(members, mems * members),
        name="tapered",
    )(slab, taper_mask, blocks)
    ensemble = gathered(gathered(gathered(own_rows, "mem", runs), "mem", strides), "mem", planes)
    update = pl.pallas_call(
        mixing_kernel,
        in_specs=[vspec(), vspec()],
        out_specs=vspec(),
        out_shape=f32(mems, tiles // mems, members, LANES),
        name="mixing",
    )(cell_state, ensemble)
    returned = lax.all_to_all(update, "mem", 0, 0, tiled=True)
    analysis = pl.pallas_call(
        add_kernel,
        in_specs=[vspec(), vspec()],
        out_specs=vspec(),
        out_shape=f32(members, rows, cols),
        name="add",
    )(forecast, returned.reshape(tiles, members, LANES))
    return analysis


def solution(mesh):
    return jax.shard_map(
        local,
        mesh=mesh,
        in_specs=(
            P("mem", "slab", None),
            P("slab", None),
            P("slab", None),
            P("slab", None),
            P("slab", None),
            P("slab"),
            P("mem", "slab"),
            P("slab", None),
            P(),
        ),
        out_specs=P("mem", "slab", None),
        check_vma=False,
    )
```

```python
import jax
import jax.numpy as jnp
from jax import lax
from jax.experimental import pallas as pl
from jax.experimental.pallas import tpu as pltpu
from jax.sharding import PartitionSpec as P


LANES = 128
PLANE = 4
RUN = 4
SLAB_SWAPS = (1, 3, 4, 12)
HIGHEST = lax.Precision.HIGHEST
SMEM = pltpu.SMEM
VMEM = pltpu.VMEM


def minmod(a, b):
    return jnp.maximum(jnp.minimum(a, b), 0.0) + jnp.minimum(jnp.maximum(a, b), 0.0)


def swap_order(swaps):
    order = [0]
    for k in swaps:
        order = order + [v ^ k for v in order]
    return order


def vspec():
    return pl.BlockSpec(memory_space=VMEM)


def sspec():
    return pl.BlockSpec(memory_space=SMEM)


def edges_kernel(first_ref, last_ref, v_ref, up_ref, down_ref):
    for r in range(2):
        up_ref[r] = first_ref[:, r, :]
        down_ref[r] = last_ref[:, 6 + r, :]
    up_ref[2] = jnp.broadcast_to(v_ref[0:1, :], up_ref.shape[1:])


def forecast_kernel(
    slab_ref, cells_ref, weights_ref, h_ref, low_ref, high_ref, u_ref, v_ref, values_ref, noise_ref, cov_ref,
    f_ref, obs_ref, white_ref,
):
    members = noise_ref.shape[0]
    rows, cols = u_ref.shape
    per_row = cols // LANES
    lane = lax.broadcasted_iota(jnp.int32, (members, cols), 1)
    at_first = lane == 0
    at_last = lane == cols - 1

    blocks = {}

    def row(r):
        if r // 8 not in blocks:
            blocks[r // 8] = jnp.swapaxes(h_ref[:, r // 8 * 8 : r // 8 * 8 + 8, :], 0, 1)
        return blocks[r // 8][r % 8]

    def columns_term(h, u):
        prev = jnp.where(at_first, 0.0, pltpu.roll(h, 1, 1))
        d = h - prev
        d_next = jnp.where(at_last, -h, pltpu.roll(d, cols - 1, 1))
        half = 0.5 * minmod(d, d_next)
        left = jnp.where(at_first, 0.0, pltpu.roll(h + half, 1, 1))
        flux = jnp.maximum(u, 0.0) * left + jnp.minimum(u, 0.0) * (h - half)
        flux_next = jnp.where(at_last, 0.0, pltpu.roll(flux, cols - 1, 1))
        return flux_next - flux

    def row_flux(v, h_low, half_low, h_high, half_high):
        return jnp.maximum(v, 0.0) * (h_low + half_low) + jnp.minimum(v, 0.0) * (h_high - half_high)

    low2, low1 = low_ref[0], low_ref[1]
    h0, h1 = row(0), row(1)
    d0, d1 = h0 - low1, h1 - h0
    half_low = 0.5 * minmod(low1 - low2, d0)
    half0 = 0.5 * minmod(d0, d1)
    flux0 = row_flux(v_ref[0:1, :], low1, half_low, h0, half0)
    carry = (h0, h1, d1, half0, flux0)
    for r in range(rows):
        h, h_up, d_up, half, flux = carry
        if r + 2 < rows:
            h_up2 = row(r + 2)
        else:
            h_up2 = high_ref[r + 2 - rows]
        v = v_ref[r + 1 : r + 2, :] if r + 1 < rows else high_ref[2, 0:1, :]
        d_up2 = h_up2 - h_up
        half_up = 0.5 * minmod(d_up, d_up2)
        flux_up = row_flux(v, h, half, h_up, half_up)
        f = h - columns_term(h, u_ref[r : r + 1, :]) - (flux_up - flux)
        for t in range(per_row):
            f_ref[r * per_row + t] = f[:, t * LANES : (t + 1) * LANES]
        carry = (h_up, h_up2, d_up2, half_up, flux_up)

    base = slab_ref[0] * (rows * cols)
    count = cells_ref.shape[0]
    foot = cells_ref.shape[1]
    lane1 = lax.broadcasted_iota(jnp.int32, (members, LANES), 1)

    def observe(o, carry):
        total, norm = carry
        acc = jnp.zeros((members, LANES), jnp.float32)
        wsum = jnp.float32(0.0)
        for k in range(foot):
            c = cells_ref[o, k] - base
            w = weights_ref[o, k].astype(jnp.float32)
            tile = f_ref[c >> 7]
            acc = acc + jnp.where(lane1 == (c & (LANES - 1)), w * tile, 0.0)
            wsum = wsum + w
        here = lane1 == o
        total = jnp.where(here, jnp.sum(acc, axis=1, keepdims=True), total)
        norm = jnp.where(here, wsum, norm)
        return total, norm

    init = jnp.zeros((members, LANES), jnp.float32)
    total, norm = lax.fori_loop(0, count, observe, (init, init + 1.0), unroll=8)
    obs = total / norm
    obs_ref[...] = obs
    innovation = values_ref[...] + noise_ref[...] - obs
    white = jnp.dot(innovation, cov_ref[...], precision=HIGHEST, preferred_element_type=jnp.float32)
    for s in range(white_ref.shape[0]):
        white_ref[s] = white[:, s * LANES : (s + 1) * LANES]


def source_z(z, t, k, depth):
    runs = depth // RUN
    run = z // RUN + (0, runs - 1, 1)[t]
    run = jnp.where(run >= runs, run - runs, run)
    return run * RUN + ((z & (RUN - 1)) ^ k)


def products_kernel(z_ref, obs_ref, white_ref, out_ref, a_ref):
    mems, members, width = a_ref.shape
    depth = mems // PLANE
    for q in range(PLANE):
        for t in range(depth // RUN):
            for k in range(RUN):
                at = ((q * depth) + t * RUN + k) * members
                a_ref[source_z(z_ref[0], t, k, depth) * PLANE + q] = obs_ref[at : at + members, :]
    a = a_ref[...].reshape(mems * members, width)
    a = a - jnp.mean(a, axis=0, keepdims=True)
    w = white_ref[0]
    for s in range(1, white_ref.shape[0]):
        w = w + white_ref[s]
    out_ref[...] = lax.dot_general(
        w, a, (((1,), (1,)), ((), ())), precision=HIGHEST, preferred_element_type=jnp.float32
    )


def tapered_kernel(slab_ref, mask_ref, own_ref, other_ref, out_ref):
    members = out_ref.shape[0]
    slab = slab_ref[0]
    order = swap_order(SLAB_SWAPS)
    half = len(order) // 2
    e = jnp.zeros(out_ref.shape, jnp.float32)
    for i, v in enumerate(order):
        ref, at = (own_ref, i) if i < half else (other_ref, i - half)
        e = e + mask_ref[slab, slab ^ v].astype(jnp.float32) * ref[at * members : (at + 1) * members, :]
    out_ref[...] = e


def mixing_kernel(z_ref, x_ref, e_ref, out_ref):
    mems, tiles, members, width = x_ref.shape
    total = mems * members
    e = e_ref[...]
    depth = mems // PLANE
    for t in range(tiles):
        x = x_ref[:, t].reshape(total, width)
        x = x - jnp.mean(x, axis=0, keepdims=True)
        u = jnp.dot(e, x, precision=HIGHEST, preferred_element_type=jnp.float32) / (total - 1)
        for q in range(PLANE):
            for r in range(depth // RUN):
                for k in range(RUN):
                    at = (q * depth + r * RUN + k) * members
                    out_ref[source_z(z_ref[0], r, k, depth) * PLANE + q, t] = u[at : at + members]


def add_kernel(f_ref, y_ref, out_ref):
    rows, cols = out_ref.shape[1:]
    per_row = cols // LANES
    for r in range(0, rows, 8):
        for t in range(per_row):
            at = [(r + i) * per_row + t for i in range(8)]
            tile = jnp.stack([f_ref[i] + y_ref[i] for i in at], 0)
            out_ref[:, r : r + 8, t * LANES : (t + 1) * LANES] = jnp.swapaxes(tile, 0, 1)


def f32(*shape):
    return jax.ShapeDtypeStruct(shape, jnp.float32)


def v32(*shape):
    return VMEM(shape, jnp.float32)


def near(x):
    return pltpu.with_memory_space_constraint(x, VMEM)


def swapped(x, axis, k):
    return lax.ppermute(x, axis, [(i, i ^ k) for i in range(lax.axis_size(axis))])


def gathered_over_mem(x, planes):
    mems = lax.axis_size("mem")
    for k in (PLANE, 2 * PLANE):
        x = jnp.concatenate([x, swapped(x, "mem", k)], 0)
    step = RUN * PLANE
    below = lax.ppermute(x, "mem", [(i, (i + step) % mems) for i in range(mems)])
    above = lax.ppermute(x, "mem", [(i, (i - step) % mems) for i in range(mems)])
    x = jnp.concatenate([x, below, above], 0)
    return lax.all_gather(x, "mem", axis=0, tiled=True, axis_index_groups=planes)


def local(
    thickness, face_u, face_v, obs_cells, obs_weights, obs_values, obs_noise, cov_inverse, taper_mask,
):
    members, rows, cols = thickness.shape
    mems = lax.axis_size("mem")
    slabs = lax.axis_size("slab")
    depth = mems // PLANE
    tiles = rows * cols // LANES
    slab = lax.axis_index("slab").astype(jnp.int32).reshape(1)
    planes = [[z * PLANE + q for q in range(PLANE)] for z in range(depth)]
    z = lax.shift_right_logical(lax.axis_index("mem").astype(jnp.int32), PLANE.bit_length() - 1).reshape(1)

    up, down = pl.pallas_call(
        edges_kernel,
        grid=(1,),
        in_specs=[
            pl.BlockSpec((members, 8, cols), lambda i: (0, 0, 0)),
            pl.BlockSpec((members, 8, cols), lambda i: (0, rows // 8 - 1, 0)),
            pl.BlockSpec((8, cols), lambda i: (0, 0)),
        ],
        out_specs=[
            pl.BlockSpec((3, members, cols), lambda i: (0, 0, 0)),
            pl.BlockSpec((2, members, cols), lambda i: (0, 0, 0)),
        ],
        out_shape=[v32(3, members, cols), v32(2, members, cols)],
        name="edges",
    )(thickness, thickness, face_v)
    low = lax.ppermute(down, "slab", [(i, i + 1) for i in range(slabs - 1)])
    high = lax.ppermute(up, "slab", [(i + 1, i) for i in range(slabs - 1)])

    forecast, obs_model, white_terms = pl.pallas_call(
        forecast_kernel,
        in_specs=[sspec(), sspec(), sspec()] + [vspec() for _ in range(8)],
        out_specs=[vspec() for _ in range(3)],
        out_shape=[v32(tiles, members, LANES), v32(members, LANES), v32(slabs, members, LANES)],
        name="forecast",
    )(
        slab, obs_cells, obs_weights, thickness, near(low), near(high), face_u, face_v,
        obs_values.reshape(1, -1), obs_noise, cov_inverse,
    )

    white_arrived = lax.all_to_all(white_terms, "slab", 0, 0, tiled=True)
    obs_all = gathered_over_mem(obs_model, planes)
    cell_state = lax.all_to_all(
        forecast.reshape(mems, tiles // mems, members, LANES), "mem", 0, 0, tiled=True
    )
    product = pl.pallas_call(
        products_kernel,
        in_specs=[sspec(), vspec(), vspec()],
        out_specs=vspec(),
        out_shape=v32(members, mems * members),
        scratch_shapes=[VMEM((mems, members, LANES), jnp.float32)],
        name="products",
    )(z, near(obs_all), near(white_arrived))
    blocks = product
    for k in SLAB_SWAPS[:-1]:
        blocks = jnp.concatenate([blocks, swapped(blocks, "slab", k)], 0)
    other_blocks = swapped(blocks, "slab", SLAB_SWAPS[-1])
    own_rows = pl.pallas_call(
        tapered_kernel,
        in_specs=[sspec(), sspec(), vspec(), vspec()],
        out_specs=vspec(),
        out_shape=v32(members, mems * members),
        name="tapered",
    )(slab, taper_mask, near(blocks), near(other_blocks))
    ensemble = gathered_over_mem(own_rows, planes)
    update = pl.pallas_call(
        mixing_kernel,
        in_specs=[sspec(), vspec(), vspec()],
        out_specs=vspec(),
        out_shape=v32(mems, tiles // mems, members, LANES),
        name="mixing",
    )(z, near(cell_state), near(ensemble))
    returned = lax.all_to_all(update, "mem", 0, 0, tiled=True)
    analysis = pl.pallas_call(
        add_kernel,
        in_specs=[vspec(), vspec()],
        out_specs=vspec(),
        out_shape=f32(members, rows, cols),
        name="add",
    )(near(forecast), near(returned.reshape(tiles, members, LANES)))
    return analysis


def solution(mesh):
    return jax.shard_map(
        local,
        mesh=mesh,
        in_specs=(
            P("mem", "slab", None),
            P("slab", None),
            P("slab", None),
            P("slab", None),
            P("slab", None),
            P("slab"),
            P("mem", "slab"),
            P("slab", None),
            P(),
        ),
        out_specs=P("mem", "slab", None),
        check_vma=False,
    )
```

```python
import jax
import jax.numpy as jnp
from jax import lax
from jax.experimental import pallas as pl
from jax.experimental.pallas import tpu as pltpu
from jax.sharding import PartitionSpec as P


LANES = 128
PLANE = 4
SLAB_SWAPS = (1, 3, 4, 12)
HIGHEST = lax.Precision.HIGHEST
SMEM = pltpu.SMEM
VMEM = pltpu.VMEM


def minmod(a, b):
    return jnp.maximum(jnp.minimum(a, b), 0.0) + jnp.minimum(jnp.maximum(a, b), 0.0)


def swap_order(swaps):
    order = [0]
    for k in swaps:
        order = order + [v ^ k for v in order]
    return order


def vspec():
    return pl.BlockSpec(memory_space=VMEM)


def sspec():
    return pl.BlockSpec(memory_space=SMEM)


def edges_kernel(first_ref, last_ref, v_ref, up_ref, down_ref):
    for r in range(2):
        up_ref[r] = first_ref[:, r, :]
        down_ref[r] = last_ref[:, 6 + r, :]
    up_ref[2] = jnp.broadcast_to(v_ref[0:1, :], up_ref.shape[1:])


def forecast_kernel(
    slab_ref, tile_ref, shift_ref, h_ref, low_ref, high_ref, u_ref, v_ref, weights_ref, values_ref, noise_ref, cov_ref,
    f_ref, near_ref, far_ref, white_ref,
):
    members = noise_ref.shape[0]
    rows, cols = u_ref.shape
    per_row = cols // LANES
    mems = f_ref.shape[0]
    tiles = f_ref.shape[1] - 1
    lane = lax.broadcasted_iota(jnp.int32, (members, cols), 1)
    at_first = lane == 0
    at_last = lane == cols - 1

    blocks = {}

    def row(r):
        if r // 8 not in blocks:
            blocks[r // 8] = jnp.swapaxes(h_ref[:, r // 8 * 8 : r // 8 * 8 + 8, :], 0, 1)
        return blocks[r // 8][r % 8]

    def columns_term(h, u):
        prev = jnp.where(at_first, 0.0, pltpu.roll(h, 1, 1))
        d = h - prev
        d_next = jnp.where(at_last, -h, pltpu.roll(d, cols - 1, 1))
        half = 0.5 * minmod(d, d_next)
        left = jnp.where(at_first, 0.0, pltpu.roll(h + half, 1, 1))
        flux = jnp.maximum(u, 0.0) * left + jnp.minimum(u, 0.0) * (h - half)
        flux_next = jnp.where(at_last, 0.0, pltpu.roll(flux, cols - 1, 1))
        return flux_next - flux

    def row_flux(v, h_low, half_low, h_high, half_high):
        return jnp.maximum(v, 0.0) * (h_low + half_low) + jnp.minimum(v, 0.0) * (h_high - half_high)

    low2, low1 = low_ref[0], low_ref[1]
    h0, h1 = row(0), row(1)
    d0, d1 = h0 - low1, h1 - h0
    half_low = 0.5 * minmod(low1 - low2, d0)
    half0 = 0.5 * minmod(d0, d1)
    flux0 = row_flux(v_ref[0:1, :], low1, half_low, h0, half0)
    carry = (h0, h1, d1, half0, flux0)
    for r in range(rows):
        h, h_up, d_up, half, flux = carry
        if r + 2 < rows:
            h_up2 = row(r + 2)
        else:
            h_up2 = high_ref[r + 2 - rows]
        v = v_ref[r + 1 : r + 2, :] if r + 1 < rows else high_ref[2, 0:1, :]
        d_up2 = h_up2 - h_up
        half_up = 0.5 * minmod(d_up, d_up2)
        flux_up = row_flux(v, h, half, h_up, half_up)
        f = h - columns_term(h, u_ref[r : r + 1, :]) - (flux_up - flux)
        for t in range(per_row):
            at = r * per_row + t
            f_ref[at // tiles, at % tiles] = f[:, t * LANES : (t + 1) * LANES]
        carry = (h_up, h_up2, d_up2, half_up, flux_up)

    foot, count = tile_ref.shape
    lane1 = lax.broadcasted_iota(jnp.int32, (members, LANES), 1)

    def observe(o, picked):
        here = lane1 == o
        out = []
        for k in range(foot):
            at = tile_ref[k, o]
            tile = f_ref[at // tiles, at % tiles]
            out.append(jnp.where(here, pltpu.roll(tile, shift_ref[k, o], 1), picked[k]))
        return tuple(out)

    zero = jnp.zeros((members, LANES), jnp.float32)
    picked = lax.fori_loop(0, count, observe, (zero,) * foot, unroll=4)
    weights = weights_ref[...].astype(jnp.float32)
    obs = picked[0] * weights[0:1]
    for k in range(1, foot):
        obs = obs + picked[k] * weights[k : k + 1]
    obs = obs / jnp.sum(weights, axis=0, keepdims=True)
    for p in range(mems):
        f_ref[p, tiles] = obs
    innovation = values_ref[...] + noise_ref[...] - obs
    white = jnp.dot(innovation, cov_ref[...], precision=HIGHEST, preferred_element_type=jnp.float32)
    order = swap_order(SLAB_SWAPS)
    blocks = white_ref
    for s in range(len(order)):
        blocks[s] = white[:, s * LANES : (s + 1) * LANES]
    half = len(order) // 2
    for i, v in enumerate(order):
        ref, at = (near_ref, i) if i < half else (far_ref, i - half)
        ref[at] = blocks[slab_ref[0] ^ v]


def products_kernel(slab_ref, mask_ref, x_ref, white_ref, swap_ref, out_ref):
    mems, tiles, members, width = x_ref.shape
    a = x_ref[:, tiles - 1].reshape(mems * members, width)
    a = a - jnp.mean(a, axis=0, keepdims=True)
    w = white_ref[...] + swap_ref[...]
    p = lax.dot_general(w, a, (((1,), (1,)), ((), ())), precision=HIGHEST, preferred_element_type=jnp.float32)
    for s in range(out_ref.shape[0]):
        out_ref[s] = mask_ref[s, slab_ref[0]].astype(jnp.float32) * p


def summed_kernel(x_ref, out_ref):
    e = x_ref[0]
    for s in range(1, x_ref.shape[0]):
        e = e + x_ref[s]
    for z in range(out_ref.shape[0]):
        out_ref[z] = e


def mixing_kernel(x_ref, e_ref, out_ref):
    mems, tiles, members, width = out_ref.shape
    total = mems * members
    e = e_ref[...]
    depth = mems // PLANE
    for t in range(tiles):
        x = x_ref[:, t].reshape(total, width)
        x = x - jnp.mean(x, axis=0, keepdims=True)
        u = jnp.dot(e, x, precision=HIGHEST, preferred_element_type=jnp.float32) / (total - 1)
        for q in range(PLANE):
            for z in range(depth):
                at = (q * depth + z) * members
                out_ref[z * PLANE + q, t] = u[at : at + members]


def add_kernel(f_ref, y_ref, out_ref):
    rows, cols = out_ref.shape[1:]
    per_row = cols // LANES
    for r in range(0, rows, 8):
        for t in range(per_row):
            at = [(r + i) * per_row + t for i in range(8)]
            tile = jnp.stack([f_ref[i // y_ref.shape[1], i % y_ref.shape[1]] + y_ref[i // y_ref.shape[1], i % y_ref.shape[1]] for i in at], 0)
            out_ref[:, r : r + 8, t * LANES : (t + 1) * LANES] = jnp.swapaxes(tile, 0, 1)


def f32(*shape):
    return jax.ShapeDtypeStruct(shape, jnp.float32)


def v32(*shape):
    return VMEM(shape, jnp.float32)


def near(x):
    return pltpu.with_memory_space_constraint(x, VMEM)


def swapped(x, axis, k):
    return lax.ppermute(x, axis, [(i, i ^ k) for i in range(lax.axis_size(axis))])


def local(
    thickness, face_u, face_v, obs_cells, obs_weights, obs_values, obs_noise, cov_inverse, taper_mask,
):
    members, rows, cols = thickness.shape
    mems = lax.axis_size("mem")
    slabs = lax.axis_size("slab")
    depth = mems // PLANE
    tiles = rows * cols // LANES // mems
    slab = lax.axis_index("slab").astype(jnp.int32).reshape(1)
    planes = [[z * PLANE + q for q in range(PLANE)] for z in range(depth)]
    columns = [[z * PLANE + q for z in range(depth)] for q in range(PLANE)]
    cells = obs_cells.T - slab * (rows * cols)
    cell_tile = lax.shift_right_logical(cells, LANES.bit_length() - 1)
    cell_shift = (lax.broadcasted_iota(jnp.int32, cells.shape, 1) - cells) & (LANES - 1)

    up, down = pl.pallas_call(
        edges_kernel,
        grid=(1,),
        in_specs=[
            pl.BlockSpec((members, 8, cols), lambda i: (0, 0, 0)),
            pl.BlockSpec((members, 8, cols), lambda i: (0, rows // 8 - 1, 0)),
            pl.BlockSpec((8, cols), lambda i: (0, 0)),
        ],
        out_specs=[
            pl.BlockSpec((3, members, cols), lambda i: (0, 0, 0)),
            pl.BlockSpec((2, members, cols), lambda i: (0, 0, 0)),
        ],
        out_shape=[v32(3, members, cols), v32(2, members, cols)],
        name="edges",
    )(thickness, thickness, face_v)
    low = lax.ppermute(down, "slab", [(i, i + 1) for i in range(slabs - 1)])
    high = lax.ppermute(up, "slab", [(i + 1, i) for i in range(slabs - 1)])

    forecast, white, white_far = pl.pallas_call(
        forecast_kernel,
        in_specs=[sspec(), sspec(), sspec()] + [vspec() for _ in range(9)],
        out_specs=[vspec() for _ in range(3)],
        out_shape=[
            v32(mems, tiles + 1, members, LANES),
            v32(slabs // 2, members, LANES),
            v32(slabs // 2, members, LANES),
        ],
        scratch_shapes=[v32(slabs, members, LANES)],
        name="forecast",
    )(
        slab, cell_tile, cell_shift, thickness, near(low), near(high), face_u, face_v, obs_weights.T,
        obs_values.reshape(1, -1), obs_noise, cov_inverse,
    )

    cell_state = lax.all_to_all(forecast, "mem", 0, 0, tiled=True)
    arrived = swapped(white_far, "slab", SLAB_SWAPS[-1])
    for k in SLAB_SWAPS[-2::-1]:
        half = white.shape[0] // 2
        white, white_far = white[:half] + arrived[:half], white[half:] + arrived[half:]
        arrived = swapped(white_far, "slab", k)
    parts = pl.pallas_call(
        products_kernel,
        in_specs=[sspec(), sspec(), vspec(), vspec(), vspec()],
        out_specs=vspec(),
        out_shape=v32(slabs, members, mems * members),
        name="products",
    )(slab, taper_mask, near(cell_state), near(white[0]), near(arrived[0]))
    parts = lax.all_to_all(parts, "slab", 0, 0, tiled=True)
    copies = pl.pallas_call(
        summed_kernel,
        in_specs=[vspec()],
        out_specs=vspec(),
        out_shape=v32(depth, members, mems * members),
        name="summed",
    )(near(parts))
    over_z = lax.all_to_all(copies, "mem", 0, 0, tiled=True, axis_index_groups=columns)
    ensemble = lax.all_gather(
        over_z.reshape(depth * members, mems * members), "mem", axis=0, tiled=True, axis_index_groups=planes
    )
    update = pl.pallas_call(
        mixing_kernel,
        in_specs=[vspec(), vspec()],
        out_specs=vspec(),
        out_shape=v32(mems, tiles, members, LANES),
        name="mixing",
    )(near(cell_state), near(ensemble))
    returned = lax.all_to_all(update, "mem", 0, 0, tiled=True)
    return pl.pallas_call(
        add_kernel,
        in_specs=[vspec(), vspec()],
        out_specs=vspec(),
        out_shape=f32(members, rows, cols),
        name="add",
    )(near(forecast), near(returned))


def solution(mesh):
    return jax.shard_map(
        local,
        mesh=mesh,
        in_specs=(
            P("mem", "slab", None),
            P("slab", None),
            P("slab", None),
            P("slab", None),
            P("slab", None),
            P("slab"),
            P("mem", "slab"),
            P("slab", None),
            P(),
        ),
        out_specs=P("mem", "slab", None),
        check_vma=False,
    )
```

```python
import jax
import jax.numpy as jnp
from jax import lax
from jax.experimental import pallas as pl
from jax.experimental.pallas import tpu as pltpu
from jax.sharding import PartitionSpec as P


LANES = 128
PLANE = 4
SLAB_SWAPS = (1, 3, 4, 12)
HIGHEST = lax.Precision.HIGHEST
ROOM = pltpu.CompilerParams(vmem_limit_bytes=12 << 20)
SMEM = pltpu.SMEM
VMEM = pltpu.VMEM


def minmod(a, b):
    return jnp.maximum(jnp.minimum(a, b), 0.0) + jnp.minimum(jnp.maximum(a, b), 0.0)


def swap_order(swaps):
    order = [0]
    for k in swaps:
        order = order + [v ^ k for v in order]
    return order


def vspec():
    return pl.BlockSpec(memory_space=VMEM)


def sspec():
    return pl.BlockSpec(memory_space=SMEM)


def edges_kernel(first_ref, last_ref, v_ref, up_ref, down_ref):
    for r in range(2):
        up_ref[r] = first_ref[:, r, :]
        down_ref[r] = last_ref[:, 6 + r, :]
    up_ref[2] = jnp.broadcast_to(v_ref[0:1, :], up_ref.shape[1:])


def forecast_kernel(
    slab_ref, spot0_ref, spot1_ref, spot2_ref, spot3_ref, h_ref, low_ref, high_ref, u_ref, v_ref, weights_ref,
    values_ref, noise_ref, cov_hbm,
    f_ref, first_ref, second_ref, near_ref, far_ref, white_ref, cov_ref, cov_sem,
):
    cov_copy = pltpu.make_async_copy(cov_hbm, cov_ref, cov_sem)
    cov_copy.start()
    members = noise_ref.shape[0]
    rows, cols = u_ref.shape
    per_row = cols // LANES
    mems, held = second_ref.shape[:2]
    tiles = 2 * held
    lane = lax.broadcasted_iota(jnp.int32, (members, cols), 1)
    at_first = lane == 0
    at_last = lane == cols - 1

    blocks = {}

    def row(r):
        if r // 8 not in blocks:
            blocks[r // 8] = jnp.swapaxes(h_ref[:, r // 8 * 8 : r // 8 * 8 + 8, :], 0, 1)
        return blocks[r // 8][r % 8]

    def columns_term(h, u):
        prev = jnp.where(at_first, 0.0, pltpu.roll(h, 1, 1))
        d = h - prev
        d_next = jnp.where(at_last, -h, pltpu.roll(d, cols - 1, 1))
        half = 0.5 * minmod(d, d_next)
        left = jnp.where(at_first, 0.0, pltpu.roll(h + half, 1, 1))
        flux = jnp.maximum(u, 0.0) * left + jnp.minimum(u, 0.0) * (h - half)
        flux_next = jnp.where(at_last, 0.0, pltpu.roll(flux, cols - 1, 1))
        return flux_next - flux

    def row_flux(v, h_low, half_low, h_high, half_high):
        return jnp.maximum(v, 0.0) * (h_low + half_low) + jnp.minimum(v, 0.0) * (h_high - half_high)

    low2, low1 = low_ref[0], low_ref[1]
    h0, h1 = row(0), row(1)
    d0, d1 = h0 - low1, h1 - h0
    half_low = 0.5 * minmod(low1 - low2, d0)
    half0 = 0.5 * minmod(d0, d1)
    flux0 = row_flux(v_ref[0:1, :], low1, half_low, h0, half0)
    carry = (h0, h1, d1, half0, flux0)
    for r in range(rows):
        h, h_up, d_up, half, flux = carry
        if r + 2 < rows:
            h_up2 = row(r + 2)
        else:
            h_up2 = high_ref[r + 2 - rows]
        v = v_ref[r + 1 : r + 2, :] if r + 1 < rows else high_ref[2, 0:1, :]
        d_up2 = h_up2 - h_up
        half_up = 0.5 * minmod(d_up, d_up2)
        flux_up = row_flux(v, h, half, h_up, half_up)
        f = h - columns_term(h, u_ref[r : r + 1, :]) - (flux_up - flux)
        for t in range(per_row):
            at = r * per_row + t
            tile = f[:, t * LANES : (t + 1) * LANES]
            f_ref[at] = tile
            if at % tiles < held:
                first_ref[at // tiles, at % tiles] = tile
            else:
                second_ref[at // tiles, at % tiles - held] = tile
        carry = (h_up, h_up2, d_up2, half_up, flux_up)

    spots = (spot0_ref, spot1_ref, spot2_ref, spot3_ref)
    foot, count = weights_ref.shape
    lane1 = lax.broadcasted_iota(jnp.int32, (members, LANES), 1)

    def observe(o, picked):
        here = lane1 == o
        out = []
        for k in range(foot):
            spot = spots[k][o]
            tile = f_ref[lax.shift_right_logical(spot, LANES.bit_length() - 1)]
            out.append(jnp.where(here, pltpu.roll(tile, spot & (LANES - 1), 1), picked[k]))
        return tuple(out)

    zero = jnp.zeros((members, LANES), jnp.float32)
    picked = lax.fori_loop(0, count, observe, (zero,) * foot, unroll=8)
    weights = weights_ref[...].astype(jnp.float32)
    obs = picked[0] * weights[0:1]
    for k in range(1, foot):
        obs = obs + picked[k] * weights[k : k + 1]
    obs = obs / jnp.sum(weights, axis=0, keepdims=True)
    for p in range(mems):
        first_ref[p, held] = obs
    innovation = values_ref[...] + noise_ref[...] - obs
    cov_copy.wait()
    white = jnp.dot(innovation, cov_ref[...], precision=HIGHEST, preferred_element_type=jnp.float32)
    order = swap_order(SLAB_SWAPS)
    blocks = white_ref
    for s in range(len(order)):
        blocks[s] = white[:, s * LANES : (s + 1) * LANES]
    half = len(order) // 2
    for i, v in enumerate(order):
        ref, at = (near_ref, i) if i < half else (far_ref, i - half)
        ref[at] = blocks[slab_ref[0] ^ v]


def products_kernel(slab_ref, mask_ref, x_ref, white_ref, swap_ref, out_ref):
    mems, tiles, members, width = x_ref.shape
    a = x_ref[:, tiles - 1].reshape(mems * members, width)
    a = a - jnp.mean(a, axis=0, keepdims=True)
    w = white_ref[...] + swap_ref[...]
    p = lax.dot_general(w, a, (((1,), (1,)), ((), ())), precision=HIGHEST, preferred_element_type=jnp.float32)
    for s in range(out_ref.shape[0]):
        out_ref[s] = mask_ref[s, slab_ref[0]].astype(jnp.float32) * p


def summed_kernel(x_ref, out_ref):
    e = x_ref[0]
    for s in range(1, x_ref.shape[0]):
        e = e + x_ref[s]
    out_ref[...] = e


def mixing_kernel(first_ref, second_ref, e_ref, out_ref):
    mems, tiles, members, width = out_ref.shape
    total = mems * members
    held = second_ref.shape[1]
    e = e_ref[...]
    depth = mems // PLANE
    for t in range(tiles):
        x = first_ref[:, t] if t < held else second_ref[:, t - held]
        x = x.reshape(total, width)
        x = x - jnp.mean(x, axis=0, keepdims=True)
        u = jnp.dot(e, x, precision=HIGHEST, preferred_element_type=jnp.float32) / (total - 1)
        for q in range(PLANE):
            for z in range(depth):
                at = (q * depth + z) * members
                out_ref[z * PLANE + q, t] = u[at : at + members]


def add_kernel(f_ref, y_ref, out_ref):
    rows, cols = out_ref.shape[1:]
    per_row = cols // LANES
    start = pl.program_id(0) * (rows * per_row)
    for r in range(0, rows, 8):
        for t in range(per_row):
            at = [start + (r + i) * per_row + t for i in range(8)]
            tile = jnp.stack([f_ref[i] + y_ref[i] for i in at], 0)
            out_ref[:, r : r + 8, t * LANES : (t + 1) * LANES] = jnp.swapaxes(tile, 0, 1)


def f32(*shape):
    return jax.ShapeDtypeStruct(shape, jnp.float32)


def v32(*shape):
    return VMEM(shape, jnp.float32)


def away(x):
    return pltpu.with_memory_space_constraint(x, pltpu.HBM)


def near(x):
    return pltpu.with_memory_space_constraint(x, VMEM)


def swapped(x, axis, k):
    return lax.ppermute(x, axis, [(i, i ^ k) for i in range(lax.axis_size(axis))])


def local(
    thickness, face_u, face_v, obs_cells, obs_weights, obs_values, obs_noise, cov_inverse, taper_mask,
):
    members, rows, cols = thickness.shape
    mems = lax.axis_size("mem")
    slabs = lax.axis_size("slab")
    depth = mems // PLANE
    tiles = rows * cols // LANES // mems
    slab = lax.axis_index("slab").astype(jnp.int32).reshape(1)
    planes = [[z * PLANE + q for q in range(PLANE)] for z in range(depth)]
    columns = [[z * PLANE + q for z in range(depth)] for q in range(PLANE)]
    cells = obs_cells.T - slab * (rows * cols)
    cell_shift = (lax.broadcasted_iota(jnp.int32, cells.shape, 1) - cells) & (LANES - 1)
    spots = (cells & -LANES) | cell_shift

    up, down = pl.pallas_call(
        edges_kernel,
        grid=(1,),
        in_specs=[
            pl.BlockSpec((members, 8, cols), lambda i: (0, 0, 0)),
            pl.BlockSpec((members, 8, cols), lambda i: (0, rows // 8 - 1, 0)),
            pl.BlockSpec((8, cols), lambda i: (0, 0)),
        ],
        out_specs=[
            pl.BlockSpec((3, members, cols), lambda i: (0, 0, 0)),
            pl.BlockSpec((2, members, cols), lambda i: (0, 0, 0)),
        ],
        out_shape=[v32(3, members, cols), v32(2, members, cols)],
        compiler_params=ROOM,
        name="edges",
    )(away(thickness), away(thickness), away(face_v))
    low = lax.ppermute(down, "slab", [(i, i + 1) for i in range(slabs - 1)])
    high = lax.ppermute(up, "slab", [(i + 1, i) for i in range(slabs - 1)])

    forecast, first, second, white, white_far = pl.pallas_call(
        forecast_kernel,
        in_specs=[sspec() for _ in range(5)] + [vspec() for _ in range(8)] + [pl.BlockSpec(memory_space=pltpu.HBM)],
        out_specs=[vspec() for _ in range(5)],
        out_shape=[
            v32(mems * tiles, members, LANES),
            v32(mems, tiles // 2 + 1, members, LANES),
            v32(mems, tiles // 2, members, LANES),
            v32(slabs // 2, members, LANES),
            v32(slabs // 2, members, LANES),
        ],
        scratch_shapes=[v32(slabs, members, LANES), v32(*cov_inverse.shape), pltpu.SemaphoreType.DMA],
        compiler_params=ROOM,
        name="forecast",
    )(
        slab, spots[0], spots[1], spots[2], spots[3], near(thickness), near(low), near(high), near(face_u),
        near(face_v), near(obs_weights.T), near(obs_values.reshape(1, -1)), near(obs_noise), away(cov_inverse),
    )

    first = lax.all_to_all(first, "mem", 0, 0, tiled=True)
    arrived = swapped(white_far, "slab", SLAB_SWAPS[-1])
    for k in SLAB_SWAPS[-2::-1]:
        half = white.shape[0] // 2
        white, white_far = white[:half] + arrived[:half], white[half:] + arrived[half:]
        arrived = swapped(white_far, "slab", k)
    parts = pl.pallas_call(
        products_kernel,
        in_specs=[sspec(), sspec(), vspec(), vspec(), vspec()],
        out_specs=vspec(),
        out_shape=v32(slabs, members, mems * members),
        compiler_params=ROOM,
        name="products",
    )(slab, taper_mask, near(first), near(white[0]), near(arrived[0]))
    parts = lax.all_to_all(parts, "slab", 0, 0, tiled=True)
    second = lax.all_to_all(second, "mem", 0, 0, tiled=True)
    own_rows = pl.pallas_call(
        summed_kernel,
        in_specs=[vspec()],
        out_specs=vspec(),
        out_shape=v32(members, mems * members),
        compiler_params=ROOM,
        name="summed",
    )(near(parts))
    ensemble = lax.all_gather(own_rows, "mem", axis=0, tiled=True, axis_index_groups=columns)
    ensemble = lax.all_gather(ensemble, "mem", axis=0, tiled=True, axis_index_groups=planes)
    update = pl.pallas_call(
        mixing_kernel,
        in_specs=[vspec(), vspec(), vspec()],
        out_specs=vspec(),
        out_shape=v32(mems, tiles, members, LANES),
        compiler_params=ROOM,
        name="mixing",
    )(near(first), near(second), near(ensemble))
    returned = lax.all_to_all(update, "mem", 0, 0, tiled=True)
    steps = 4
    return pl.pallas_call(
        add_kernel,
        grid=(steps,),
        in_specs=[vspec(), vspec()],
        out_specs=pl.BlockSpec((members, rows // steps, cols), lambda i: (0, i, 0)),
        out_shape=f32(members, rows, cols),
        compiler_params=ROOM,
        name="add",
    )(near(forecast), near(returned.reshape(mems * tiles, members, LANES)))


def solution(mesh):
    return jax.shard_map(
        local,
        mesh=mesh,
        in_specs=(
            P("mem", "slab", None),
            P("slab", None),
            P("slab", None),
            P("slab", None),
            P("slab", None),
            P("slab"),
            P("mem", "slab"),
            P("slab", None),
            P(),
        ),
        out_specs=P("mem", "slab", None),
        check_vma=False,
    )
```

```python
import jax
import jax.numpy as jnp
from jax import lax
from jax.experimental import pallas as pl
from jax.experimental.pallas import tpu as pltpu
from jax.sharding import PartitionSpec as P


LANES = 128
PLANE = 4
RUN = 4
COLUMN = 4
HIGHEST = lax.Precision.HIGHEST
ROOM = pltpu.CompilerParams(vmem_limit_bytes=12 << 20)
SMEM = pltpu.SMEM
VMEM = pltpu.VMEM


def minmod(a, b):
    return jnp.maximum(jnp.minimum(a, b), 0.0) + jnp.minimum(jnp.maximum(a, b), 0.0)


def vspec():
    return pl.BlockSpec(memory_space=VMEM)


def sspec():
    return pl.BlockSpec(memory_space=SMEM)


def edges_kernel(first_ref, last_ref, v_ref, up_ref, down_ref):
    for r in range(2):
        up_ref[r] = first_ref[:, r, :]
        down_ref[r] = last_ref[:, 6 + r, :]
    up_ref[2] = jnp.broadcast_to(v_ref[0:1, :], up_ref.shape[1:])


def forecast_kernel(
    slab_ref, spot0_ref, spot1_ref, spot2_ref, spot3_ref, h_ref, low_ref, high_ref, u_ref, v_ref, weights_ref,
    values_ref, noise_ref, cov_hbm,
    f_ref, obs_ref, white0_ref, white1_ref, white2_ref, white3_ref, stack_ref, cov_ref, cov_sem,
):
    cov_copy = pltpu.make_async_copy(cov_hbm, cov_ref, cov_sem)
    cov_copy.start()
    members = noise_ref.shape[0]
    rows, cols = u_ref.shape
    per_row = cols // LANES
    batch = 8
    lane = lax.broadcasted_iota(jnp.int32, (members * batch, cols), 1)
    at_first = lane == 0
    at_last = lane == cols - 1

    blocks = {}

    def row(r):
        if r // 8 not in blocks:
            blocks[r // 8] = jnp.swapaxes(h_ref[:, r // 8 * 8 : r // 8 * 8 + 8, :], 0, 1)
        return blocks[r // 8][r % 8]

    def columns_term(h, u):
        prev = jnp.where(at_first, 0.0, pltpu.roll(h, 1, 1))
        d = h - prev
        d_next = jnp.where(at_last, -h, pltpu.roll(d, cols - 1, 1))
        half = 0.5 * minmod(d, d_next)
        left = jnp.where(at_first, 0.0, pltpu.roll(h + half, 1, 1))
        flux = jnp.maximum(u, 0.0) * left + jnp.minimum(u, 0.0) * (h - half)
        flux_next = jnp.where(at_last, 0.0, pltpu.roll(flux, cols - 1, 1))
        return flux_next - flux

    def row_flux(v, h_low, half_low, h_high, half_high):
        return jnp.maximum(v, 0.0) * (h_low + half_low) + jnp.minimum(v, 0.0) * (h_high - half_high)

    low2, low1 = low_ref[0], low_ref[1]
    h0, h1 = row(0), row(1)
    d0, d1 = h0 - low1, h1 - h0
    half_low = 0.5 * minmod(low1 - low2, d0)
    half0 = 0.5 * minmod(d0, d1)
    flux0 = row_flux(v_ref[0:1, :], low1, half_low, h0, half0)
    carry = (h0, h1, d1, half0, flux0)
    for r in range(rows):
        h, h_up, d_up, half, flux = carry
        if r + 2 < rows:
            h_up2 = row(r + 2)
        else:
            h_up2 = high_ref[r + 2 - rows]
        v = v_ref[r + 1 : r + 2, :] if r + 1 < rows else high_ref[2, 0:1, :]
        d_up2 = h_up2 - h_up
        half_up = 0.5 * minmod(d_up, d_up2)
        flux_up = row_flux(v, h, half, h_up, half_up)
        if r % batch == 0:
            inside = range(r, r + batch)
            term = columns_term(
                jnp.concatenate([row(i) for i in inside], 0),
                jnp.concatenate([jnp.broadcast_to(u_ref[i : i + 1, :], (members, cols)) for i in inside], 0),
            )
        f = h - term[r % batch * members : (r % batch + 1) * members] - (flux_up - flux)
        for t in range(per_row):
            f_ref[r * per_row + t] = f[:, t * LANES : (t + 1) * LANES]
        carry = (h_up, h_up2, d_up2, half_up, flux_up)

    spots = (spot0_ref, spot1_ref, spot2_ref, spot3_ref)
    foot, count = weights_ref.shape
    lane1 = lax.broadcasted_iota(jnp.int32, (members, LANES), 1)

    def observe(o, picked):
        here = lane1 == o
        out = []
        for k in range(foot):
            spot = spots[k][o]
            tile = f_ref[lax.shift_right_logical(spot, LANES.bit_length() - 1)]
            out.append(jnp.where(here, pltpu.roll(tile, spot & (LANES - 1), 1), picked[k]))
        return tuple(out)

    zero = jnp.zeros((members, LANES), jnp.float32)
    picked = lax.fori_loop(0, count, observe, (zero,) * foot, unroll=8)
    weights = weights_ref[...].astype(jnp.float32)
    obs = picked[0] * weights[0:1]
    for k in range(1, foot):
        obs = obs + picked[k] * weights[k : k + 1]
    obs = obs / jnp.sum(weights, axis=0, keepdims=True)
    for p in range(obs_ref.shape[0]):
        obs_ref[p] = obs
    innovation = values_ref[...] + noise_ref[...] - obs
    cov_copy.wait()
    white = jnp.dot(innovation, cov_ref[...], precision=HIGHEST, preferred_element_type=jnp.float32)
    groups = (white0_ref, white1_ref, white2_ref, white3_ref)
    for s in range(len(groups) * COLUMN):
        stack_ref[s] = white[:, s * LANES : (s + 1) * LANES]
    for k, ref in enumerate(groups):
        for i in range(COLUMN):
            ref[i] = stack_ref[slab_ref[0] ^ (k * COLUMN + i)]


def halved_kernel(x0_ref, x1_ref, x2_ref, x3_ref, out0_ref, out1_ref, out2_ref, out3_ref):
    for i, ref in enumerate((out0_ref, out1_ref, out2_ref, out3_ref)):
        ref[...] = x0_ref[i] + x1_ref[i] + x2_ref[i] + x3_ref[i]


def source_z(z, t, k, depth):
    runs = depth // RUN
    run = lax.shift_right_logical(z, RUN.bit_length() - 1) + (0, runs - 1, 1)[t]
    run = jnp.where(run >= runs, run - runs, run)
    return run * RUN + ((z & (RUN - 1)) ^ k)


def products_kernel(slab_ref, mask_ref, obs_ref, w0_ref, w1_ref, w2_ref, w3_ref, out_ref):
    mems, members, width = obs_ref.shape
    a = obs_ref[...].reshape(mems * members, width)
    a = a - jnp.mean(a, axis=0, keepdims=True)
    w = w0_ref[...] + w1_ref[...] + w2_ref[...] + w3_ref[...]
    p = lax.dot_general(w, a, (((1,), (1,)), ((), ())), precision=HIGHEST, preferred_element_type=jnp.float32)
    for s in range(out_ref.shape[0]):
        out_ref[s] = mask_ref[s, slab_ref[0]].astype(jnp.float32) * p


def summed_kernel(x_ref, out_ref):
    e = x_ref[0]
    for s in range(1, x_ref.shape[0]):
        e = e + x_ref[s]
    out_ref[...] = e


def mixing_kernel(z_ref, x_ref, e_ref, out_ref):
    mems, tiles, members, width = x_ref.shape
    total = mems * members
    depth = mems // PLANE
    e = e_ref[...]
    for t in range(tiles):
        x = x_ref[:, t].reshape(total, width)
        x = x - jnp.mean(x, axis=0, keepdims=True)
        u = jnp.dot(e, x, precision=HIGHEST, preferred_element_type=jnp.float32) / (total - 1)
        for q in range(PLANE):
            for r in range(depth // RUN):
                for k in range(RUN):
                    at = (q * depth + r * RUN + k) * members
                    out_ref[source_z(z_ref[0], r, k, depth) * PLANE + q, t] = u[at : at + members]


def add_kernel(f_ref, y_ref, out_ref):
    rows, cols = out_ref.shape[1:]
    per_row = cols // LANES
    start = pl.program_id(0) * (rows * per_row)
    for r in range(0, rows, 8):
        for t in range(per_row):
            at = [start + (r + i) * per_row + t for i in range(8)]
            tile = jnp.stack([f_ref[i] + y_ref[i] for i in at], 0)
            out_ref[:, r : r + 8, t * LANES : (t + 1) * LANES] = jnp.swapaxes(tile, 0, 1)


def f32(*shape):
    return jax.ShapeDtypeStruct(shape, jnp.float32)


def v32(*shape):
    return VMEM(shape, jnp.float32)


def away(x):
    return pltpu.with_memory_space_constraint(x, pltpu.HBM)


def near(x):
    return pltpu.with_memory_space_constraint(x, VMEM)


def swapped(x, axis, k):
    return lax.ppermute(x, axis, [(i, i ^ k) for i in range(lax.axis_size(axis))])


def shifted(x, axis, k):
    count = lax.axis_size(axis)
    return lax.ppermute(x, axis, [(i, (i + k) % count) for i in range(count)])


def local(
    thickness, face_u, face_v, obs_cells, obs_weights, obs_values, obs_noise, cov_inverse, taper_mask,
):
    members, rows, cols = thickness.shape
    mems = lax.axis_size("mem")
    slabs = lax.axis_size("slab")
    depth = mems // PLANE
    tiles = rows * cols // LANES // mems
    slab = lax.axis_index("slab").astype(jnp.int32).reshape(1)
    planes = [[z * PLANE + q for q in range(PLANE)] for z in range(depth)]
    z = lax.shift_right_logical(lax.axis_index("mem").astype(jnp.int32), PLANE.bit_length() - 1).reshape(1)
    cells = obs_cells.T - slab * (rows * cols)
    cell_shift = (lax.broadcasted_iota(jnp.int32, cells.shape, 1) - cells) & (LANES - 1)
    spots = (cells & -LANES) | cell_shift

    up, down = pl.pallas_call(
        edges_kernel,
        grid=(1,),
        in_specs=[
            pl.BlockSpec((members, 8, cols), lambda i: (0, 0, 0)),
            pl.BlockSpec((members, 8, cols), lambda i: (0, rows // 8 - 1, 0)),
            pl.BlockSpec((8, cols), lambda i: (0, 0)),
        ],
        out_specs=[
            pl.BlockSpec((3, members, cols), lambda i: (0, 0, 0)),
            pl.BlockSpec((2, members, cols), lambda i: (0, 0, 0)),
        ],
        out_shape=[v32(3, members, cols), v32(2, members, cols)],
        compiler_params=ROOM,
        name="edges",
    )(away(thickness), away(thickness), away(face_v))
    low = lax.ppermute(down, "slab", [(i, i + 1) for i in range(slabs - 1)])
    high = lax.ppermute(up, "slab", [(i + 1, i) for i in range(slabs - 1)])

    forecast, obs_copies, *white = pl.pallas_call(
        forecast_kernel,
        in_specs=[sspec() for _ in range(5)] + [vspec() for _ in range(8)] + [pl.BlockSpec(memory_space=pltpu.HBM)],
        out_specs=[vspec() for _ in range(6)],
        out_shape=[v32(mems * tiles, members, LANES), v32(mems, members, LANES)]
        + [v32(COLUMN, members, LANES) for _ in range(4)],
        scratch_shapes=[v32(slabs, members, LANES), v32(*cov_inverse.shape), pltpu.SemaphoreType.DMA],
        compiler_params=ROOM,
        name="forecast",
    )(
        slab, spots[0], spots[1], spots[2], spots[3], near(thickness), near(low), near(high), near(face_u),
        near(face_v), near(obs_weights.T), near(obs_values.reshape(1, -1)), near(obs_noise), away(cov_inverse),
    )

    obs_all = lax.all_to_all(obs_copies, "mem", 0, 0, tiled=True)
    arrived = [swapped(white[k], "slab", k * COLUMN) for k in (1, 3, 2)]
    white = pl.pallas_call(
        halved_kernel,
        in_specs=[vspec() for _ in range(4)],
        out_specs=[vspec() for _ in range(4)],
        out_shape=[v32(members, LANES) for _ in range(4)],
        compiler_params=ROOM,
        name="halved",
    )(near(white[0]), *[near(x) for x in arrived])
    arrived = [swapped(white[k], "slab", k) for k in (1, 3, 2)]
    parts = pl.pallas_call(
        products_kernel,
        in_specs=[sspec(), sspec()] + [vspec() for _ in range(5)],
        out_specs=vspec(),
        out_shape=v32(slabs, members, mems * members),
        compiler_params=ROOM,
        name="products",
    )(slab, taper_mask, near(obs_all), near(white[0]), *[near(x) for x in arrived])
    parts = lax.all_to_all(parts, "slab", 0, 0, tiled=True)
    cell_state = lax.all_to_all(forecast.reshape(mems, tiles, members, LANES), "mem", 0, 0, tiled=True)
    own_rows = pl.pallas_call(
        summed_kernel,
        in_specs=[vspec()],
        out_specs=vspec(),
        out_shape=v32(members, mems * members),
        compiler_params=ROOM,
        name="summed",
    )(near(parts))
    run = jnp.concatenate([own_rows] + [swapped(own_rows, "mem", k * PLANE) for k in range(1, RUN)], 0)
    below, above = shifted(run, "mem", RUN * PLANE), shifted(run, "mem", -RUN * PLANE)
    ensemble = jnp.concatenate([run, below, above], 0)
    ensemble = lax.all_gather(ensemble, "mem", axis=0, tiled=True, axis_index_groups=planes)
    update = pl.pallas_call(
        mixing_kernel,
        in_specs=[sspec(), vspec(), vspec()],
        out_specs=vspec(),
        out_shape=v32(mems, tiles, members, LANES),
        compiler_params=ROOM,
        name="mixing",
    )(z, near(cell_state), near(ensemble))
    returned = lax.all_to_all(update, "mem", 0, 0, tiled=True)
    steps = 4
    return pl.pallas_call(
        add_kernel,
        grid=(steps,),
        in_specs=[vspec(), vspec()],
        out_specs=pl.BlockSpec((members, rows // steps, cols), lambda i: (0, i, 0)),
        out_shape=f32(members, rows, cols),
        compiler_params=ROOM,
        name="add",
    )(near(forecast), near(returned.reshape(mems * tiles, members, LANES)))


def solution(mesh):
    return jax.shard_map(
        local,
        mesh=mesh,
        in_specs=(
            P("mem", "slab", None),
            P("slab", None),
            P("slab", None),
            P("slab", None),
            P("slab", None),
            P("slab"),
            P("mem", "slab"),
            P("slab", None),
            P(),
        ),
        out_specs=P("mem", "slab", None),
        check_vma=False,
    )
```

```python
import jax
import jax.numpy as jnp
from jax import lax
from jax.experimental import pallas as pl
from jax.experimental.pallas import tpu as pltpu
from jax.sharding import PartitionSpec as P


LANES = 128
PLANE = 4
SLAB_SWAPS = (1, 3, 4, 12)
HIGHEST = lax.Precision.HIGHEST
ROOM = pltpu.CompilerParams(vmem_limit_bytes=12 << 20)
SMEM = pltpu.SMEM
VMEM = pltpu.VMEM


def minmod(a, b):
    return jnp.maximum(jnp.minimum(a, b), 0.0) + jnp.minimum(jnp.maximum(a, b), 0.0)


def swap_order(swaps):
    order = [0]
    for k in swaps:
        order = order + [v ^ k for v in order]
    return order


def vspec():
    return pl.BlockSpec(memory_space=VMEM)


def sspec():
    return pl.BlockSpec(memory_space=SMEM)


def edges_kernel(first_ref, last_ref, v_ref, up_ref, down_ref):
    for r in range(2):
        up_ref[r] = first_ref[:, r, :]
        down_ref[r] = last_ref[:, 6 + r, :]
    up_ref[2] = jnp.broadcast_to(v_ref[0:1, :], up_ref.shape[1:])


def forecast_kernel(
    slab_ref, spot0_ref, spot1_ref, spot2_ref, spot3_ref, h_ref, low_ref, high_ref, u_ref, v_ref, weights_ref,
    values_ref, noise_ref, cov_hbm,
    f_ref, pieces_ref, near_ref, far_ref, stack_ref, cov_ref, cov_sem,
):
    cov_copy = pltpu.make_async_copy(cov_hbm, cov_ref, cov_sem)
    cov_copy.start()
    members = noise_ref.shape[0]
    rows, cols = u_ref.shape
    per_row = cols // LANES
    mems, tiles = pieces_ref.shape[0], pieces_ref.shape[1] - 1
    batch = 8
    lane = lax.broadcasted_iota(jnp.int32, (members * batch, cols), 1)
    at_first = lane == 0
    at_last = lane == cols - 1

    blocks = {}

    def row(r):
        if r // 8 not in blocks:
            blocks[r // 8] = jnp.swapaxes(h_ref[:, r // 8 * 8 : r // 8 * 8 + 8, :], 0, 1)
        return blocks[r // 8][r % 8]

    def columns_term(h, u):
        prev = jnp.where(at_first, 0.0, pltpu.roll(h, 1, 1))
        d = h - prev
        d_next = jnp.where(at_last, -h, pltpu.roll(d, cols - 1, 1))
        half = 0.5 * minmod(d, d_next)
        left = jnp.where(at_first, 0.0, pltpu.roll(h + half, 1, 1))
        flux = jnp.maximum(u, 0.0) * left + jnp.minimum(u, 0.0) * (h - half)
        flux_next = jnp.where(at_last, 0.0, pltpu.roll(flux, cols - 1, 1))
        return flux_next - flux

    def row_flux(v, h_low, half_low, h_high, half_high):
        return jnp.maximum(v, 0.0) * (h_low + half_low) + jnp.minimum(v, 0.0) * (h_high - half_high)

    low2, low1 = low_ref[0], low_ref[1]
    h0, h1 = row(0), row(1)
    d0, d1 = h0 - low1, h1 - h0
    half_low = 0.5 * minmod(low1 - low2, d0)
    half0 = 0.5 * minmod(d0, d1)
    flux0 = row_flux(v_ref[0:1, :], low1, half_low, h0, half0)
    carry = (h0, h1, d1, half0, flux0)
    for r in range(rows):
        h, h_up, d_up, half, flux = carry
        if r + 2 < rows:
            h_up2 = row(r + 2)
        else:
            h_up2 = high_ref[r + 2 - rows]
        v = v_ref[r + 1 : r + 2, :] if r + 1 < rows else high_ref[2, 0:1, :]
        d_up2 = h_up2 - h_up
        half_up = 0.5 * minmod(d_up, d_up2)
        flux_up = row_flux(v, h, half, h_up, half_up)
        if r % batch == 0:
            inside = range(r, r + batch)
            term = columns_term(
                jnp.concatenate([row(i) for i in inside], 0),
                jnp.concatenate([jnp.broadcast_to(u_ref[i : i + 1, :], (members, cols)) for i in inside], 0),
            )
        f = h - term[r % batch * members : (r % batch + 1) * members] - (flux_up - flux)
        for t in range(per_row):
            at = r * per_row + t
            tile = f[:, t * LANES : (t + 1) * LANES]
            f_ref[at] = tile
            pieces_ref[at // tiles, at % tiles] = tile
        carry = (h_up, h_up2, d_up2, half_up, flux_up)

    spots = (spot0_ref, spot1_ref, spot2_ref, spot3_ref)
    foot, count = weights_ref.shape
    lane1 = lax.broadcasted_iota(jnp.int32, (members, LANES), 1)

    def observe(o, picked):
        here = lane1 == o
        out = []
        for k in range(foot):
            spot = spots[k][o]
            tile = f_ref[lax.shift_right_logical(spot, LANES.bit_length() - 1)]
            out.append(jnp.where(here, pltpu.roll(tile, spot & (LANES - 1), 1), picked[k]))
        return tuple(out)

    zero = jnp.zeros((members, LANES), jnp.float32)
    picked = lax.fori_loop(0, count, observe, (zero,) * foot, unroll=8)
    weights = weights_ref[...].astype(jnp.float32)
    obs = picked[0] * weights[0:1]
    for k in range(1, foot):
        obs = obs + picked[k] * weights[k : k + 1]
    obs = obs / jnp.sum(weights, axis=0, keepdims=True)
    for p in range(mems):
        pieces_ref[p, tiles] = obs
    innovation = values_ref[...] + noise_ref[...] - obs
    cov_copy.wait()
    white = jnp.dot(innovation, cov_ref[...], precision=HIGHEST, preferred_element_type=jnp.float32)
    order = swap_order(SLAB_SWAPS)
    for s in range(len(order)):
        stack_ref[s] = white[:, s * LANES : (s + 1) * LANES]
    half = len(order) // 2
    for i, v in enumerate(order):
        ref, at = (near_ref, i) if i < half else (far_ref, i - half)
        ref[at] = stack_ref[slab_ref[0] ^ v]


def products_kernel(slab_ref, mask_ref, x_ref, white_ref, swap_ref, out_ref):
    mems, tiles, members, width = x_ref.shape
    a = x_ref[:, tiles - 1].reshape(mems * members, width)
    a = a - jnp.mean(a, axis=0, keepdims=True)
    w = white_ref[...] + swap_ref[...]
    p = lax.dot_general(w, a, (((1,), (1,)), ((), ())), precision=HIGHEST, preferred_element_type=jnp.float32)
    for s in range(out_ref.shape[0]):
        out_ref[s] = mask_ref[s, slab_ref[0]].astype(jnp.float32) * p


def summed_kernel(x_ref, out_ref):
    e = x_ref[0]
    for s in range(1, x_ref.shape[0]):
        e = e + x_ref[s]
    for z in range(out_ref.shape[0]):
        out_ref[z] = e


def mixing_kernel(x_ref, e_ref, out_ref):
    mems, tiles, members, width = out_ref.shape
    total = mems * members
    e = e_ref[...]
    depth = mems // PLANE
    for t in range(tiles):
        x = x_ref[:, t].reshape(total, width)
        x = x - jnp.mean(x, axis=0, keepdims=True)
        u = jnp.dot(e, x, precision=HIGHEST, preferred_element_type=jnp.float32) / (total - 1)
        for q in range(PLANE):
            for z in range(depth):
                at = (q * depth + z) * members
                out_ref[z * PLANE + q, t] = u[at : at + members]


def add_kernel(f_ref, y_ref, out_ref):
    rows, cols = out_ref.shape[1:]
    per_row = cols // LANES
    start = pl.program_id(0) * (rows * per_row)
    for r in range(0, rows, 8):
        for t in range(per_row):
            at = [start + (r + i) * per_row + t for i in range(8)]
            tile = jnp.stack([f_ref[i] + y_ref[i] for i in at], 0)
            out_ref[:, r : r + 8, t * LANES : (t + 1) * LANES] = jnp.swapaxes(tile, 0, 1)


def f32(*shape):
    return jax.ShapeDtypeStruct(shape, jnp.float32)


def v32(*shape):
    return VMEM(shape, jnp.float32)


def away(x):
    return pltpu.with_memory_space_constraint(x, pltpu.HBM)


def near(x):
    return pltpu.with_memory_space_constraint(x, VMEM)


def swapped(x, axis, k):
    return lax.ppermute(x, axis, [(i, i ^ k) for i in range(lax.axis_size(axis))])


def local(
    thickness, face_u, face_v, obs_cells, obs_weights, obs_values, obs_noise, cov_inverse, taper_mask,
):
    members, rows, cols = thickness.shape
    mems = lax.axis_size("mem")
    slabs = lax.axis_size("slab")
    depth = mems // PLANE
    tiles = rows * cols // LANES // mems
    slab = lax.axis_index("slab").astype(jnp.int32).reshape(1)
    planes = [[z * PLANE + q for q in range(PLANE)] for z in range(depth)]
    columns = [[z * PLANE + q for z in range(depth)] for q in range(PLANE)]
    cells = obs_cells.T - slab * (rows * cols)
    cell_shift = (lax.broadcasted_iota(jnp.int32, cells.shape, 1) - cells) & (LANES - 1)
    spots = (cells & -LANES) | cell_shift

    up, down = pl.pallas_call(
        edges_kernel,
        grid=(1,),
        in_specs=[
            pl.BlockSpec((members, 8, cols), lambda i: (0, 0, 0)),
            pl.BlockSpec((members, 8, cols), lambda i: (0, rows // 8 - 1, 0)),
            pl.BlockSpec((8, cols), lambda i: (0, 0)),
        ],
        out_specs=[
            pl.BlockSpec((3, members, cols), lambda i: (0, 0, 0)),
            pl.BlockSpec((2, members, cols), lambda i: (0, 0, 0)),
        ],
        out_shape=[v32(3, members, cols), v32(2, members, cols)],
        compiler_params=ROOM,
        name="edges",
    )(away(thickness), away(thickness), away(face_v))
    low = lax.ppermute(down, "slab", [(i, i + 1) for i in range(slabs - 1)])
    high = lax.ppermute(up, "slab", [(i + 1, i) for i in range(slabs - 1)])

    forecast, pieces, white, white_far = pl.pallas_call(
        forecast_kernel,
        in_specs=[sspec() for _ in range(5)] + [vspec() for _ in range(8)] + [pl.BlockSpec(memory_space=pltpu.HBM)],
        out_specs=[vspec() for _ in range(4)],
        out_shape=[v32(mems * tiles, members, LANES), v32(mems, tiles + 1, members, LANES)]
        + [v32(slabs // 2, members, LANES) for _ in range(2)],
        scratch_shapes=[v32(slabs, members, LANES), v32(*cov_inverse.shape), pltpu.SemaphoreType.DMA],
        compiler_params=ROOM,
        name="forecast",
    )(
        slab, spots[0], spots[1], spots[2], spots[3], near(thickness), near(low), near(high), near(face_u),
        near(face_v), near(obs_weights.T), near(obs_values.reshape(1, -1)), near(obs_noise), away(cov_inverse),
    )

    cell_state = lax.all_to_all(pieces, "mem", 0, 0, tiled=True)
    arrived = swapped(white_far, "slab", SLAB_SWAPS[-1])
    for k in SLAB_SWAPS[-2::-1]:
        half = white.shape[0] // 2
        white, white_far = white[:half] + arrived[:half], white[half:] + arrived[half:]
        arrived = swapped(white_far, "slab", k)
    parts = pl.pallas_call(
        products_kernel,
        in_specs=[sspec(), sspec(), vspec(), vspec(), vspec()],
        out_specs=vspec(),
        out_shape=v32(slabs, members, mems * members),
        compiler_params=ROOM,
        name="products",
    )(slab, taper_mask, near(cell_state), near(white[0]), near(arrived[0]))
    parts = lax.all_to_all(parts, "slab", 0, 0, tiled=True)
    copies = pl.pallas_call(
        summed_kernel,
        in_specs=[vspec()],
        out_specs=vspec(),
        out_shape=v32(depth, members, mems * members),
        compiler_params=ROOM,
        name="summed",
    )(near(parts))
    over_z = lax.all_to_all(copies, "mem", 0, 0, tiled=True, axis_index_groups=columns)
    ensemble = lax.all_gather(
        over_z.reshape(depth * members, mems * members), "mem", axis=0, tiled=True, axis_index_groups=planes
    )
    update = pl.pallas_call(
        mixing_kernel,
        in_specs=[vspec(), vspec()],
        out_specs=vspec(),
        out_shape=v32(mems, tiles, members, LANES),
        compiler_params=ROOM,
        name="mixing",
    )(near(cell_state), near(ensemble))
    returned = lax.all_to_all(update, "mem", 0, 0, tiled=True)
    steps = 4
    return pl.pallas_call(
        add_kernel,
        grid=(steps,),
        in_specs=[vspec(), vspec()],
        out_specs=pl.BlockSpec((members, rows // steps, cols), lambda i: (0, i, 0)),
        out_shape=f32(members, rows, cols),
        compiler_params=ROOM,
        name="add",
    )(near(forecast), near(returned.reshape(mems * tiles, members, LANES)))


def solution(mesh):
    return jax.shard_map(
        local,
        mesh=mesh,
        in_specs=(
            P("mem", "slab", None),
            P("slab", None),
            P("slab", None),
            P("slab", None),
            P("slab", None),
            P("slab"),
            P("mem", "slab"),
            P("slab", None),
            P(),
        ),
        out_specs=P("mem", "slab", None),
        check_vma=False,
    )
```

```python
import jax
import jax.numpy as jnp
from jax import lax
from jax.experimental import pallas as pl
from jax.experimental.pallas import tpu as pltpu
from jax.sharding import PartitionSpec as P


LANES = 128
PLANE = 4
SLAB_SWAPS = (1, 3, 4, 12)
HIGHEST = lax.Precision.HIGHEST
ROOM = pltpu.CompilerParams(vmem_limit_bytes=12 << 20)
SMEM = pltpu.SMEM
VMEM = pltpu.VMEM


def minmod(a, b):
    return jnp.maximum(jnp.minimum(a, b), 0.0) + jnp.minimum(jnp.maximum(a, b), 0.0)


def swap_order(swaps):
    order = [0]
    for k in swaps:
        order = order + [v ^ k for v in order]
    return order


def vspec():
    return pl.BlockSpec(memory_space=VMEM)


def sspec():
    return pl.BlockSpec(memory_space=SMEM)


def edges_kernel(first_ref, last_ref, v_ref, up_ref, down_ref):
    for r in range(2):
        up_ref[r] = first_ref[:, r, :]
        down_ref[r] = last_ref[:, 6 + r, :]
    up_ref[2] = jnp.broadcast_to(v_ref[0:1, :], up_ref.shape[1:])


def row_flux(v, h_low, half_low, h_high, half_high):
    return jnp.maximum(v, 0.0) * (h_low + half_low) + jnp.minimum(v, 0.0) * (h_high - half_high)


def inner_kernel(h_ref, u_ref, v_ref, f_ref, rim_ref):
    members, rows, cols = h_ref.shape
    per_row = cols // LANES
    batch = 8
    lane = lax.broadcasted_iota(jnp.int32, (members * batch, cols), 1)
    at_first = lane == 0
    at_last = lane == cols - 1
    blocks = {}

    def row(r):
        if r // 8 not in blocks:
            blocks[r // 8] = jnp.swapaxes(h_ref[:, r // 8 * 8 : r // 8 * 8 + 8, :], 0, 1)
        return blocks[r // 8][r % 8]

    def columns_term(h, u):
        prev = jnp.where(at_first, 0.0, pltpu.roll(h, 1, 1))
        d = h - prev
        d_next = jnp.where(at_last, -h, pltpu.roll(d, cols - 1, 1))
        half = 0.5 * minmod(d, d_next)
        left = jnp.where(at_first, 0.0, pltpu.roll(h + half, 1, 1))
        flux = jnp.maximum(u, 0.0) * left + jnp.minimum(u, 0.0) * (h - half)
        flux_next = jnp.where(at_last, 0.0, pltpu.roll(flux, cols - 1, 1))
        return flux_next - flux

    h, h_up = row(2), row(3)
    d_up = h_up - h
    half1 = 0.5 * minmod(row(1) - row(0), h - row(1))
    half = 0.5 * minmod(h - row(1), d_up)
    carry = (h, h_up, d_up, half, row_flux(v_ref[2:3, :], row(1), half1, h, half))
    for r in range(rows):
        if r % batch == 0:
            inside = range(r, r + batch)
            term = columns_term(
                jnp.concatenate([row(i) for i in inside], 0),
                jnp.concatenate([jnp.broadcast_to(u_ref[i : i + 1, :], (members, cols)) for i in inside], 0),
            )
        f = row(r) - term[r % batch * members : (r % batch + 1) * members]
        if 2 <= r < rows - 2:
            h, h_up, d_up, half, flux = carry
            h_up2 = row(r + 2)
            d_up2 = h_up2 - h_up
            half_up = 0.5 * minmod(d_up, d_up2)
            flux_up = row_flux(v_ref[r + 1 : r + 2, :], h, half, h_up, half_up)
            f = f - (flux_up - flux)
            carry = (h_up, h_up2, d_up2, half_up, flux_up)
        for t in range(per_row):
            f_ref[r * per_row + t] = f[:, t * LANES : (t + 1) * LANES]
    for i in range(4):
        rim_ref[i] = row(i)
        rim_ref[4 + i] = row(rows - 4 + i)


def forecast_kernel(
    slab_ref, spot0_ref, spot1_ref, spot2_ref, spot3_ref, inner_ref, rim_ref, low_ref, high_ref, v_ref, weights_ref,
    values_ref, noise_ref, cov_hbm,
    f_ref, pieces_ref, near_ref, far_ref, stack_ref, cov_ref, cov_sem,
):
    cov_copy = pltpu.make_async_copy(cov_hbm, cov_ref, cov_sem)
    cov_copy.start()
    members = noise_ref.shape[0]
    rows, cols = v_ref.shape
    per_row = cols // LANES
    mems, tiles = pieces_ref.shape[0], pieces_ref.shape[1] - 1

    def edge_terms(h, v):
        half = [0.5 * minmod(h[i] - h[i - 1], h[i + 1] - h[i]) for i in range(1, 5)]
        flux = [row_flux(v[i], h[i + 1], half[i], h[i + 2], half[i + 1]) for i in range(3)]
        return flux[1] - flux[0], flux[2] - flux[1]

    lows = edge_terms(
        [low_ref[0], low_ref[1], rim_ref[0], rim_ref[1], rim_ref[2], rim_ref[3]],
        [v_ref[i : i + 1, :] for i in range(3)],
    )
    highs = edge_terms(
        [rim_ref[4], rim_ref[5], rim_ref[6], rim_ref[7], high_ref[0], high_ref[1]],
        [v_ref[rows - 2 : rows - 1, :], v_ref[rows - 1 : rows, :], high_ref[2, 0:1, :]],
    )
    late = {0: lows[0], 1: lows[1], rows - 2: highs[0], rows - 1: highs[1]}
    for r in range(rows):
        for t in range(per_row):
            at = r * per_row + t
            tile = inner_ref[at]
            if r in late:
                tile = tile - late[r][:, t * LANES : (t + 1) * LANES]
            f_ref[at] = tile
            pieces_ref[at // tiles, at % tiles] = tile

    spots = (spot0_ref, spot1_ref, spot2_ref, spot3_ref)
    foot, count = weights_ref.shape
    lane1 = lax.broadcasted_iota(jnp.int32, (members, LANES), 1)

    def observe(o, picked):
        here = lane1 == o
        out = []
        for k in range(foot):
            spot = spots[k][o]
            tile = f_ref[lax.shift_right_logical(spot, LANES.bit_length() - 1)]
            out.append(jnp.where(here, pltpu.roll(tile, spot & (LANES - 1), 1), picked[k]))
        return tuple(out)

    zero = jnp.zeros((members, LANES), jnp.float32)
    picked = lax.fori_loop(0, count, observe, (zero,) * foot, unroll=8)
    weights = weights_ref[...].astype(jnp.float32)
    obs = picked[0] * weights[0:1]
    for k in range(1, foot):
        obs = obs + picked[k] * weights[k : k + 1]
    obs = obs / jnp.sum(weights, axis=0, keepdims=True)
    for p in range(mems):
        pieces_ref[p, tiles] = obs
    innovation = values_ref[...] + noise_ref[...] - obs
    cov_copy.wait()
    white = jnp.dot(innovation, cov_ref[...], precision=HIGHEST, preferred_element_type=jnp.float32)
    order = swap_order(SLAB_SWAPS)
    for s in range(len(order)):
        stack_ref[s] = white[:, s * LANES : (s + 1) * LANES]
    half = len(order) // 2
    for i, v in enumerate(order):
        ref, at = (near_ref, i) if i < half else (far_ref, i - half)
        ref[at] = stack_ref[slab_ref[0] ^ v]


def products_kernel(slab_ref, mask_ref, x_ref, white_ref, swap_ref, out_ref):
    mems, tiles, members, width = x_ref.shape
    a = x_ref[:, tiles - 1].reshape(mems * members, width)
    a = a - jnp.mean(a, axis=0, keepdims=True)
    w = white_ref[...] + swap_ref[...]
    p = lax.dot_general(w, a, (((1,), (1,)), ((), ())), precision=HIGHEST, preferred_element_type=jnp.float32)
    for s in range(out_ref.shape[0]):
        out_ref[s] = mask_ref[s, slab_ref[0]].astype(jnp.float32) * p


def summed_kernel(x_ref, out_ref):
    e = x_ref[0]
    for s in range(1, x_ref.shape[0]):
        e = e + x_ref[s]
    for z in range(out_ref.shape[0]):
        out_ref[z] = e


def two_parts(x):
    high = x.astype(jnp.bfloat16)
    return high, (x - high.astype(jnp.float32)).astype(jnp.bfloat16)


def product(a, b):
    return jnp.dot(a, b, preferred_element_type=jnp.float32)


def mixing_kernel(x_ref, e_ref, out_ref):
    mems, tiles, members, width = out_ref.shape
    total = mems * members
    e_high, e_low = two_parts(e_ref[...])
    depth = mems // PLANE
    for t in range(tiles):
        x = x_ref[:, t].reshape(total, width)
        x_high, x_low = two_parts(x - jnp.mean(x, axis=0, keepdims=True))
        u = product(e_high, x_high) + (product(e_high, x_low) + product(e_low, x_high))
        u = u / (total - 1)
        for q in range(PLANE):
            for z in range(depth):
                at = (q * depth + z) * members
                out_ref[z * PLANE + q, t] = u[at : at + members]


def add_kernel(f_ref, y_ref, out_ref):
    rows, cols = out_ref.shape[1:]
    per_row = cols // LANES
    start = pl.program_id(0) * (rows * per_row)
    for r in range(0, rows, 8):
        for t in range(per_row):
            at = [start + (r + i) * per_row + t for i in range(8)]
            tile = jnp.stack([f_ref[i] + y_ref[i] for i in at], 0)
            out_ref[:, r : r + 8, t * LANES : (t + 1) * LANES] = jnp.swapaxes(tile, 0, 1)


def f32(*shape):
    return jax.ShapeDtypeStruct(shape, jnp.float32)


def v32(*shape):
    return VMEM(shape, jnp.float32)


def away(x):
    return pltpu.with_memory_space_constraint(x, pltpu.HBM)


def near(x):
    return pltpu.with_memory_space_constraint(x, VMEM)


def swapped(x, axis, k):
    return lax.ppermute(x, axis, [(i, i ^ k) for i in range(lax.axis_size(axis))])


def local(
    thickness, face_u, face_v, obs_cells, obs_weights, obs_values, obs_noise, cov_inverse, taper_mask,
):
    members, rows, cols = thickness.shape
    mems = lax.axis_size("mem")
    slabs = lax.axis_size("slab")
    depth = mems // PLANE
    tiles = rows * cols // LANES // mems
    slab = lax.axis_index("slab").astype(jnp.int32).reshape(1)
    planes = [[z * PLANE + q for q in range(PLANE)] for z in range(depth)]
    columns = [[z * PLANE + q for z in range(depth)] for q in range(PLANE)]
    cells = obs_cells.T - slab * (rows * cols)
    cell_shift = (lax.broadcasted_iota(jnp.int32, cells.shape, 1) - cells) & (LANES - 1)
    spots = (cells & -LANES) | cell_shift

    up, down = pl.pallas_call(
        edges_kernel,
        grid=(1,),
        in_specs=[
            pl.BlockSpec((members, 8, cols), lambda i: (0, 0, 0)),
            pl.BlockSpec((members, 8, cols), lambda i: (0, rows // 8 - 1, 0)),
            pl.BlockSpec((8, cols), lambda i: (0, 0)),
        ],
        out_specs=[
            pl.BlockSpec((3, members, cols), lambda i: (0, 0, 0)),
            pl.BlockSpec((2, members, cols), lambda i: (0, 0, 0)),
        ],
        out_shape=[v32(3, members, cols), v32(2, members, cols)],
        compiler_params=ROOM,
        name="edges",
    )(away(thickness), away(thickness), away(face_v))
    low = lax.ppermute(down, "slab", [(i, i + 1) for i in range(slabs - 1)])
    high = lax.ppermute(up, "slab", [(i + 1, i) for i in range(slabs - 1)])
    speed = near(face_v)
    inner, rim = pl.pallas_call(
        inner_kernel,
        in_specs=[vspec() for _ in range(3)],
        out_specs=[vspec() for _ in range(2)],
        out_shape=[v32(mems * tiles, members, LANES), v32(8, members, cols)],
        compiler_params=ROOM,
        name="inner",
    )(near(thickness), near(face_u), speed)

    forecast, pieces, white, white_far = pl.pallas_call(
        forecast_kernel,
        in_specs=[sspec() for _ in range(5)] + [vspec() for _ in range(8)] + [pl.BlockSpec(memory_space=pltpu.HBM)],
        out_specs=[vspec() for _ in range(4)],
        out_shape=[v32(mems * tiles, members, LANES), v32(mems, tiles + 1, members, LANES)]
        + [v32(slabs // 2, members, LANES) for _ in range(2)],
        scratch_shapes=[v32(slabs, members, LANES), v32(*cov_inverse.shape), pltpu.SemaphoreType.DMA],
        compiler_params=ROOM,
        name="forecast",
    )(
        slab, spots[0], spots[1], spots[2], spots[3], near(inner), near(rim), near(low), near(high), speed,
        near(obs_weights.T), near(obs_values.reshape(1, -1)), near(obs_noise), away(cov_inverse),
    )

    cell_state = lax.all_to_all(pieces, "mem", 0, 0, tiled=True)
    arrived = swapped(white_far, "slab", SLAB_SWAPS[-1])
    for k in SLAB_SWAPS[-2::-1]:
        half = white.shape[0] // 2
        white, white_far = white[:half] + arrived[:half], white[half:] + arrived[half:]
        arrived = swapped(white_far, "slab", k)
    parts = pl.pallas_call(
        products_kernel,
        in_specs=[sspec(), sspec(), vspec(), vspec(), vspec()],
        out_specs=vspec(),
        out_shape=v32(slabs, members, mems * members),
        compiler_params=ROOM,
        name="products",
    )(slab, taper_mask, near(cell_state), near(white[0]), near(arrived[0]))
    parts = lax.all_to_all(parts, "slab", 0, 0, tiled=True)
    copies = pl.pallas_call(
        summed_kernel,
        in_specs=[vspec()],
        out_specs=vspec(),
        out_shape=v32(depth, members, mems * members),
        compiler_params=ROOM,
        name="summed",
    )(near(parts))
    over_z = lax.all_to_all(copies, "mem", 0, 0, tiled=True, axis_index_groups=columns)
    ensemble = lax.all_gather(
        over_z.reshape(depth * members, mems * members), "mem", axis=0, tiled=True, axis_index_groups=planes
    )
    update = pl.pallas_call(
        mixing_kernel,
        in_specs=[vspec(), vspec()],
        out_specs=vspec(),
        out_shape=v32(mems, tiles, members, LANES),
        compiler_params=ROOM,
        name="mixing",
    )(near(cell_state), near(ensemble))
    returned = lax.all_to_all(update, "mem", 0, 0, tiled=True)
    steps = 4
    return pl.pallas_call(
        add_kernel,
        grid=(steps,),
        in_specs=[vspec(), vspec()],
        out_specs=pl.BlockSpec((members, rows // steps, cols), lambda i: (0, i, 0)),
        out_shape=f32(members, rows, cols),
        compiler_params=ROOM,
        name="add",
    )(near(forecast), near(returned.reshape(mems * tiles, members, LANES)))


def solution(mesh):
    return jax.shard_map(
        local,
        mesh=mesh,
        in_specs=(
            P("mem", "slab", None),
            P("slab", None),
            P("slab", None),
            P("slab", None),
            P("slab", None),
            P("slab"),
            P("mem", "slab"),
            P("slab", None),
            P(),
        ),
        out_specs=P("mem", "slab", None),
        check_vma=False,
    )
```

```python
import jax
import jax.numpy as jnp
from jax import lax
from jax.experimental import pallas as pl
from jax.experimental.pallas import tpu as pltpu
from jax.sharding import PartitionSpec as P


LANES = 128
PLANE = 4
SLAB_SWAPS = (1, 3, 4, 12)
HIGHEST = lax.Precision.HIGHEST
ROOM = pltpu.CompilerParams(vmem_limit_bytes=12 << 20)
SMEM = pltpu.SMEM
VMEM = pltpu.VMEM


def minmod(a, b):
    return jnp.maximum(jnp.minimum(a, b), 0.0) + jnp.minimum(jnp.maximum(a, b), 0.0)


def swap_order(swaps):
    order = [0]
    for k in swaps:
        order = order + [v ^ k for v in order]
    return order


def vspec():
    return pl.BlockSpec(memory_space=VMEM)


def sspec():
    return pl.BlockSpec(memory_space=SMEM)


def edges_kernel(first_ref, last_ref, v_ref, up_ref, down_ref):
    for r in range(2):
        up_ref[r] = first_ref[:, r, :]
        down_ref[r] = last_ref[:, 6 + r, :]
    up_ref[2] = jnp.broadcast_to(v_ref[0:1, :], up_ref.shape[1:])


def row_flux(v, h_low, half_low, h_high, half_high):
    return jnp.maximum(v, 0.0) * (h_low + half_low) + jnp.minimum(v, 0.0) * (h_high - half_high)


def inner_kernel(h_ref, u_ref, v_ref, values_ref, noise_ref, weights_ref, f_ref, rim_ref, seen_ref, share_ref):
    members, rows, cols = h_ref.shape
    per_row = cols // LANES
    batch = 8
    lane = lax.broadcasted_iota(jnp.int32, (members * batch, cols), 1)
    at_first = lane == 0
    at_last = lane == cols - 1
    blocks = {}

    def row(r):
        if r // 8 not in blocks:
            blocks[r // 8] = jnp.swapaxes(h_ref[:, r // 8 * 8 : r // 8 * 8 + 8, :], 0, 1)
        return blocks[r // 8][r % 8]

    def columns_term(h, u):
        prev = jnp.where(at_first, 0.0, pltpu.roll(h, 1, 1))
        d = h - prev
        d_next = jnp.where(at_last, -h, pltpu.roll(d, cols - 1, 1))
        half = 0.5 * minmod(d, d_next)
        left = jnp.where(at_first, 0.0, pltpu.roll(h + half, 1, 1))
        flux = jnp.maximum(u, 0.0) * left + jnp.minimum(u, 0.0) * (h - half)
        flux_next = jnp.where(at_last, 0.0, pltpu.roll(flux, cols - 1, 1))
        return flux_next - flux

    h, h_up = row(2), row(3)
    d_up = h_up - h
    half1 = 0.5 * minmod(row(1) - row(0), h - row(1))
    half = 0.5 * minmod(h - row(1), d_up)
    carry = (h, h_up, d_up, half, row_flux(v_ref[2:3, :], row(1), half1, h, half))
    for r in range(rows):
        if r % batch == 0:
            inside = range(r, r + batch)
            term = columns_term(
                jnp.concatenate([row(i) for i in inside], 0),
                jnp.concatenate([jnp.broadcast_to(u_ref[i : i + 1, :], (members, cols)) for i in inside], 0),
            )
        f = row(r) - term[r % batch * members : (r % batch + 1) * members]
        if 2 <= r < rows - 2:
            h, h_up, d_up, half, flux = carry
            h_up2 = row(r + 2)
            d_up2 = h_up2 - h_up
            half_up = 0.5 * minmod(d_up, d_up2)
            flux_up = row_flux(v_ref[r + 1 : r + 2, :], h, half, h_up, half_up)
            f = f - (flux_up - flux)
            carry = (h_up, h_up2, d_up2, half_up, flux_up)
        for t in range(per_row):
            f_ref[r * per_row + t] = f[:, t * LANES : (t + 1) * LANES]
    seen_ref[...] = values_ref[...] + noise_ref[...]
    share_ref[...] = weights_ref[...].astype(jnp.float32)
    for i in range(4):
        rim_ref[i] = row(i)
        rim_ref[4 + i] = row(rows - 4 + i)


def forecast_kernel(
    slab_ref, spot0_ref, spot1_ref, spot2_ref, spot3_ref, inner_ref, rim_ref, low_ref, high_ref, v_ref, weights_ref,
    seen_ref, cov_hbm,
    f_ref, pieces_ref, near_ref, far_ref, stack_ref, cov_ref, cov_sem,
):
    cov_copy = pltpu.make_async_copy(cov_hbm, cov_ref, cov_sem)
    cov_copy.start()
    members = seen_ref.shape[0]
    rows, cols = v_ref.shape
    per_row = cols // LANES
    mems, tiles = pieces_ref.shape[0], pieces_ref.shape[1] - 1

    def edge_terms(h, v):
        half = [0.5 * minmod(h[i] - h[i - 1], h[i + 1] - h[i]) for i in range(1, 5)]
        flux = [row_flux(v[i], h[i + 1], half[i], h[i + 2], half[i + 1]) for i in range(3)]
        return flux[1] - flux[0], flux[2] - flux[1]

    lows = edge_terms(
        [low_ref[0], low_ref[1], rim_ref[0], rim_ref[1], rim_ref[2], rim_ref[3]],
        [v_ref[i : i + 1, :] for i in range(3)],
    )
    highs = edge_terms(
        [rim_ref[4], rim_ref[5], rim_ref[6], rim_ref[7], high_ref[0], high_ref[1]],
        [v_ref[rows - 2 : rows - 1, :], v_ref[rows - 1 : rows, :], high_ref[2, 0:1, :]],
    )
    late = {0: lows[0], 1: lows[1], rows - 2: highs[0], rows - 1: highs[1]}
    for r in range(rows):
        for t in range(per_row):
            at = r * per_row + t
            tile = inner_ref[at]
            if r in late:
                tile = tile - late[r][:, t * LANES : (t + 1) * LANES]
            f_ref[at] = tile
            pieces_ref[at // tiles, at % tiles] = tile

    spots = (spot0_ref, spot1_ref, spot2_ref, spot3_ref)
    foot, count = weights_ref.shape
    lane1 = lax.broadcasted_iota(jnp.int32, (members, LANES), 1)

    def observe(o, picked):
        here = lane1 == o
        out = []
        for k in range(foot):
            spot = spots[k][o]
            tile = f_ref[lax.shift_right_logical(spot, LANES.bit_length() - 1)]
            out.append(jnp.where(here, pltpu.roll(tile, spot & (LANES - 1), 1), picked[k]))
        return tuple(out)

    zero = jnp.zeros((members, LANES), jnp.float32)
    picked = lax.fori_loop(0, count, observe, (zero,) * foot, unroll=8)
    weights = weights_ref[...]
    obs = picked[0] * weights[0:1]
    for k in range(1, foot):
        obs = obs + picked[k] * weights[k : k + 1]
    obs = obs / jnp.sum(weights, axis=0, keepdims=True)
    for p in range(mems):
        pieces_ref[p, tiles] = obs
    innovation = seen_ref[...] - obs
    cov_copy.wait()
    white = jnp.dot(innovation, cov_ref[...], precision=HIGHEST, preferred_element_type=jnp.float32)
    order = swap_order(SLAB_SWAPS)
    for s in range(len(order)):
        stack_ref[s] = white[:, s * LANES : (s + 1) * LANES]
    half = len(order) // 2
    for i, v in enumerate(order):
        ref, at = (near_ref, i) if i < half else (far_ref, i - half)
        ref[at] = stack_ref[slab_ref[0] ^ v]


def products_kernel(slab_ref, mask_ref, x_ref, white_ref, swap_ref, out_ref):
    mems, tiles, members, width = x_ref.shape
    a = x_ref[:, tiles - 1].reshape(mems * members, width)
    a = a - jnp.mean(a, axis=0, keepdims=True)
    w = white_ref[...] + swap_ref[...]
    p = lax.dot_general(w, a, (((1,), (1,)), ((), ())), precision=HIGHEST, preferred_element_type=jnp.float32)
    for s in range(out_ref.shape[0]):
        out_ref[s] = mask_ref[s, slab_ref[0]].astype(jnp.float32) * p


def summed_kernel(x_ref, out_ref):
    e = x_ref[0]
    for s in range(1, x_ref.shape[0]):
        e = e + x_ref[s]
    for z in range(out_ref.shape[0]):
        out_ref[z] = e


def two_parts(x):
    high = x.astype(jnp.bfloat16)
    return high, (x - high.astype(jnp.float32)).astype(jnp.bfloat16)


def product(a, b):
    return jnp.dot(a, b, preferred_element_type=jnp.float32)


def mixing_kernel(x_ref, e_ref, out_ref):
    mems, tiles, members, width = out_ref.shape
    total = mems * members
    e_high, e_low = two_parts(e_ref[...])
    depth = mems // PLANE
    for t in range(tiles):
        x = x_ref[:, t].reshape(total, width)
        x_high, x_low = two_parts(x - jnp.mean(x, axis=0, keepdims=True))
        u = product(e_high, x_high) + (product(e_high, x_low) + product(e_low, x_high))
        u = u / (total - 1)
        for q in range(PLANE):
            for z in range(depth):
                at = (q * depth + z) * members
                out_ref[z * PLANE + q, t] = u[at : at + members]


def add_kernel(f_ref, y_ref, out_ref):
    rows, cols = out_ref.shape[1:]
    per_row = cols // LANES
    start = pl.program_id(0) * (rows * per_row)
    for r in range(0, rows, 8):
        for t in range(per_row):
            at = [start + (r + i) * per_row + t for i in range(8)]
            tile = jnp.stack([f_ref[i] + y_ref[i] for i in at], 0)
            out_ref[:, r : r + 8, t * LANES : (t + 1) * LANES] = jnp.swapaxes(tile, 0, 1)


def f32(*shape):
    return jax.ShapeDtypeStruct(shape, jnp.float32)


def v32(*shape):
    return VMEM(shape, jnp.float32)


def away(x):
    return pltpu.with_memory_space_constraint(x, pltpu.HBM)


def near(x):
    return pltpu.with_memory_space_constraint(x, VMEM)


def swapped(x, axis, k):
    return lax.ppermute(x, axis, [(i, i ^ k) for i in range(lax.axis_size(axis))])


def local(
    thickness, face_u, face_v, obs_cells, obs_weights, obs_values, obs_noise, cov_inverse, taper_mask,
):
    members, rows, cols = thickness.shape
    mems = lax.axis_size("mem")
    slabs = lax.axis_size("slab")
    depth = mems // PLANE
    tiles = rows * cols // LANES // mems
    slab = lax.axis_index("slab").astype(jnp.int32).reshape(1)
    planes = [[z * PLANE + q for q in range(PLANE)] for z in range(depth)]
    columns = [[z * PLANE + q for z in range(depth)] for q in range(PLANE)]
    cells = obs_cells.T - slab * (rows * cols)
    cell_shift = (lax.broadcasted_iota(jnp.int32, cells.shape, 1) - cells) & (LANES - 1)
    spots = (cells & -LANES) | cell_shift

    up, down = pl.pallas_call(
        edges_kernel,
        grid=(1,),
        in_specs=[
            pl.BlockSpec((members, 8, cols), lambda i: (0, 0, 0)),
            pl.BlockSpec((members, 8, cols), lambda i: (0, rows // 8 - 1, 0)),
            pl.BlockSpec((8, cols), lambda i: (0, 0)),
        ],
        out_specs=[
            pl.BlockSpec((3, members, cols), lambda i: (0, 0, 0)),
            pl.BlockSpec((2, members, cols), lambda i: (0, 0, 0)),
        ],
        out_shape=[v32(3, members, cols), v32(2, members, cols)],
        compiler_params=ROOM,
        name="edges",
    )(away(thickness), away(thickness), away(face_v))
    low = lax.ppermute(down, "slab", [(i, i + 1) for i in range(slabs - 1)])
    high = lax.ppermute(up, "slab", [(i + 1, i) for i in range(slabs - 1)])
    speed = near(face_v)
    inner, rim, seen, share = pl.pallas_call(
        inner_kernel,
        in_specs=[vspec() for _ in range(6)],
        out_specs=[vspec() for _ in range(4)],
        out_shape=[
            v32(mems * tiles, members, LANES),
            v32(8, members, cols),
            v32(members, LANES),
            v32(*obs_weights.T.shape),
        ],
        compiler_params=ROOM,
        name="inner",
    )(near(thickness), near(face_u), speed, obs_values.reshape(1, -1), obs_noise, obs_weights.T)

    forecast, pieces, white, white_far = pl.pallas_call(
        forecast_kernel,
        in_specs=[sspec() for _ in range(5)] + [vspec() for _ in range(7)] + [pl.BlockSpec(memory_space=pltpu.HBM)],
        out_specs=[vspec() for _ in range(4)],
        out_shape=[v32(mems * tiles, members, LANES), v32(mems, tiles + 1, members, LANES)]
        + [v32(slabs // 2, members, LANES) for _ in range(2)],
        scratch_shapes=[v32(slabs, members, LANES), v32(*cov_inverse.shape), pltpu.SemaphoreType.DMA],
        compiler_params=ROOM,
        name="forecast",
    )(
        slab, spots[0], spots[1], spots[2], spots[3], near(inner), near(rim), near(low), near(high), speed,
        near(share), near(seen), away(cov_inverse),
    )

    cell_state = lax.all_to_all(pieces, "mem", 0, 0, tiled=True)
    arrived = swapped(white_far, "slab", SLAB_SWAPS[-1])
    for k in SLAB_SWAPS[-2::-1]:
        half = white.shape[0] // 2
        white, white_far = white[:half] + arrived[:half], white[half:] + arrived[half:]
        arrived = swapped(white_far, "slab", k)
    parts = pl.pallas_call(
        products_kernel,
        in_specs=[sspec(), sspec(), vspec(), vspec(), vspec()],
        out_specs=vspec(),
        out_shape=v32(slabs, members, mems * members),
        compiler_params=ROOM,
        name="products",
    )(slab, taper_mask, near(cell_state), near(white[0]), near(arrived[0]))
    parts = lax.all_to_all(parts, "slab", 0, 0, tiled=True)
    copies = pl.pallas_call(
        summed_kernel,
        in_specs=[vspec()],
        out_specs=vspec(),
        out_shape=v32(depth, members, mems * members),
        compiler_params=ROOM,
        name="summed",
    )(near(parts))
    over_z = lax.all_to_all(copies, "mem", 0, 0, tiled=True, axis_index_groups=columns)
    ensemble = lax.all_gather(
        over_z.reshape(depth * members, mems * members), "mem", axis=0, tiled=True, axis_index_groups=planes
    )
    update = pl.pallas_call(
        mixing_kernel,
        in_specs=[vspec(), vspec()],
        out_specs=vspec(),
        out_shape=v32(mems, tiles, members, LANES),
        compiler_params=ROOM,
        name="mixing",
    )(near(cell_state), near(ensemble))
    returned = lax.all_to_all(update, "mem", 0, 0, tiled=True)
    steps = 4
    return pl.pallas_call(
        add_kernel,
        grid=(steps,),
        in_specs=[vspec(), vspec()],
        out_specs=pl.BlockSpec((members, rows // steps, cols), lambda i: (0, i, 0)),
        out_shape=f32(members, rows, cols),
        compiler_params=ROOM,
        name="add",
    )(near(forecast), near(returned.reshape(mems * tiles, members, LANES)))


def solution(mesh):
    return jax.shard_map(
        local,
        mesh=mesh,
        in_specs=(
            P("mem", "slab", None),
            P("slab", None),
            P("slab", None),
            P("slab", None),
            P("slab", None),
            P("slab"),
            P("mem", "slab"),
            P("slab", None),
            P(),
        ),
        out_specs=P("mem", "slab", None),
        check_vma=False,
    )
```
